32 devices in a mesh: ta: 2 (over x), gz: 4 (over y, core), gy: 4 (over z).
Axes of the slice: x: 2, y: 2, z: 4, core: 2. Of those that a mesh axis runs over, the one named last changes fastest.
Arguments:
- propagator: bfloat16 [2, 4, 3, 12, 2, 4, 512], P(None, None, None, None, 'ta', 'gz', 'gy'), may hold values from -6 to 6
- links: bfloat16 [2, 3, 3, 2, 4, 512], P(None, None, None, 'ta', 'gz', 'gy'), may hold values from -2.5 to 2.5
- source_z: int32 [2, 4], replicated, may hold values from 0 to 3
- displacements: int32 [3], replicated, may hold values from 0 to 2, each once
- momenta: int32 [4], replicated, may hold values from 1 to 3
- gamma_perm: int32 [4, 4], replicated, may hold values from 0 to 3, each once within a row
- gamma_phase: int32 [4, 4], replicated, may hold values from 0 to 3
Outputs:
- correlator: float32 [2, 3, 4, 4, 2], replicated
The draws below stay inside these ranges and needn't reach their ends.
Inputs may be any that keep to these rules, and one draw needn't show every extreme that they name: `displacements`: every displacement from -1 to 1 appears exactly once. `gamma_perm`: each row is a permutation of the four spin indices.
All inputs are finite; a program needn't handle non-finite values.
Results may differ from the reference program's by a relative error of at most 0.0003.
Values may be sent and summed in bfloat16 or wider, within the bound.
No kernel may reach another device: no remote copies, remote signals or barrier semaphores. Data moves between devices by JAX's collectives and lax.ppermute only.
A program may use at most 64 MiB of HBM per device.

```python
import math
import jax
import jax.numpy as jnp
from jax import lax

NX = 64
NG = 4
NP = 4
NSTEP = 1
NDISP = 3
NT = 2
NZ = 4
NY = 8
NYX = 512


def with_ends(array, rng, least, largest):
    longest = array.shape.index(max(array.shape))
    spots = []
    for shift in (0, 1):
        where = [jax.random.randint(jax.random.fold_in(rng, axis), (), 0, length) for axis, length in enumerate(array.shape)]
        where[longest] = (where[longest] + shift) % array.shape[longest]
        spots.append(tuple(where))
    return array.at[spots[0]].set(least).at[spots[1]].set(largest)


def block_levels(rng, dims, shards, least, high):
    level, own = 1.0, jax.random.fold_in(rng, 6)
    for axis_at, blocks in shards:
        steps = jnp.exp(jax.random.uniform(jax.random.fold_in(own, axis_at), (blocks,), jnp.float32, least / len(shards), high / len(shards)))
        level = level * jnp.repeat(steps, dims[axis_at] // blocks).reshape([-1 if axis == axis_at else 1 for axis in range(len(dims))])
    return level


def centred(own_key, extent, width, most, split=(), held_as=jnp.bfloat16):
    gain = block_levels(own_key, extent, split, -0.22, 0.18) if split else 1.0
    array = jax.random.normal(own_key, extent, jnp.float32) * width * gain
    return jnp.minimum(jnp.maximum(array, -most), most).astype(held_as)


def setup_inputs(seed: int = 0) -> dict:
    key_of = jax.random.split(jax.random.key(seed), 8)
    return {
        "propagator": centred(key_of[0], (2, 4, 3, 12, NT, NZ, NYX), 1.0, 6.0, ((4, 2), (5, 4), (6, 4))),
        "links": centred(key_of[1], (2, 3, 3, NT, NZ, NYX), 6 ** -0.5, 2.5, ((3, 2), (4, 4), (5, 4))),
        "source_z": with_ends(jax.random.randint(key_of[2], (NT, NP), 0, NZ), jax.random.fold_in(key_of[2], 1), 0, NZ - 1).astype(jnp.int32),
        "displacements": jax.random.permutation(key_of[3], NDISP).astype(jnp.int32),
        "momenta": with_ends(jax.random.randint(key_of[4], (NP,), 1, 4), jax.random.fold_in(key_of[4], 1), 1, 3).astype(jnp.int32),
        "gamma_perm": jax.vmap(lambda own: jax.random.permutation(own, 4))(jax.random.split(key_of[5], NG)).reshape((NG, 4)).astype(jnp.int32),
        "gamma_phase": with_ends(jax.random.randint(key_of[6], (NG, 4), 0, 4), jax.random.fold_in(key_of[6], 1), 0, 3).astype(jnp.int32),
    }


highest = lax.Precision.HIGHEST

def colour_apply(wilson, field_now):
    form = 'ab...,sbc...->sac...'
    real_part = jnp.einsum(form, wilson[0], field_now[0], precision=highest) - jnp.einsum(form, wilson[1], field_now[1], precision=highest)
    imag_part = jnp.einsum(form, wilson[0], field_now[1], precision=highest) + jnp.einsum(form, wilson[1], field_now[0], precision=highest)
    return jnp.stack([real_part, imag_part])

def link_product(left_link, right_link):
    form = 'ab...,bc...->ac...'
    real_part = jnp.einsum(form, left_link[0], right_link[0], precision=highest) - jnp.einsum(form, left_link[1], right_link[1], precision=highest)
    imag_part = jnp.einsum(form, left_link[0], right_link[1], precision=highest) + jnp.einsum(form, left_link[1], right_link[0], precision=highest)
    return jnp.stack([real_part, imag_part])

def dagger(link_field):
    return jnp.stack([jnp.swapaxes(link_field[0], 0, 1), -jnp.swapaxes(link_field[1], 0, 1)])

def spin_pairs(source, field_now):
    form = 'sac...,uac...->su...'
    real_part = jnp.einsum(form, source[0], field_now[0], precision=highest) + jnp.einsum(form, source[1], field_now[1], precision=highest)
    imag_part = jnp.einsum(form, source[0], field_now[1], precision=highest) - jnp.einsum(form, source[1], field_now[0], precision=highest)
    return (real_part, imag_part)

def insert(gamma_real, gamma_imag, pairs):
    pair_real, pair_imag = pairs
    form = 'gsu,su...->g...'
    real_part = jnp.einsum(form, gamma_real, pair_real, precision=highest) - jnp.einsum(form, gamma_imag, pair_imag, precision=highest)
    imag_part = jnp.einsum(form, gamma_real, pair_imag, precision=highest) + jnp.einsum(form, gamma_imag, pair_real, precision=highest)
    return (real_part, imag_part)

def gamma_tables(gamma_perm, gamma_phase):
    columns = jnp.arange(4, dtype=jnp.int32)
    hits = (gamma_perm[:, :, None] == columns[None, None, :]).astype(jnp.float32)
    real_part = (gamma_phase == 0).astype(jnp.float32) - (gamma_phase == 2).astype(jnp.float32)
    imag_part = (gamma_phase == 1).astype(jnp.float32) - (gamma_phase == 3).astype(jnp.float32)
    return (hits * real_part[:, :, None], hits * imag_part[:, :, None])

def reference(propagator, links, source_z, displacements, momenta, gamma_perm, gamma_phase):
    gamma_real, gamma_imag = gamma_tables(gamma_perm, gamma_phase)
    depth_index = jnp.arange(NZ, dtype=jnp.int32)
    turn_count = momenta[None, :, None] * (depth_index[None, None, :] - source_z[:, :, None]) % NZ
    angles = turn_count.astype(jnp.float32) * (2.0 * math.pi / NZ)
    cosine_all = jnp.cos(angles)
    sine_all = jnp.sin(angles)
    scaling = 1.0 / (24.0 * math.sqrt(NX * NY * NZ))
    unit = jnp.broadcast_to(jnp.eye(3, dtype=jnp.float32)[:, :, None, None], (3, 3, NZ, NYX))
    identity = jnp.stack([unit, jnp.zeros_like(unit)])

    def one_slice(slice_pack):
        source = slice_pack[0].astype(jnp.float32)
        link_field = slice_pack[1].astype(jnp.float32)
        cosine = slice_pack[2]
        sine_table = slice_pack[3]

        def project(field_now):
            trace_real, trace_imag = insert(gamma_real, gamma_imag, spin_pairs(source, field_now))
            line_real = lax.optimization_barrier(jnp.sum(trace_real, axis=-1))
            line_imag = lax.optimization_barrier(jnp.sum(trace_imag, axis=-1))
            real_part = jnp.dot(line_real, cosine.T, precision=highest) + jnp.dot(line_imag, sine_table.T, precision=highest)
            imag_part = jnp.dot(line_imag, cosine.T, precision=highest) - jnp.dot(line_real, sine_table.T, precision=highest)
            return jnp.stack([real_part, imag_part], axis=-1) * scaling
        results = {0: project(source)}
        wilson = identity
        for reach in range(1, NSTEP + 1):
            wilson = link_product(wilson, jnp.roll(link_field, -(reach - 1), axis=3))
            results[reach] = project(colour_apply(wilson, jnp.roll(source, -reach, axis=4)))
        wilson = identity
        for reach in range(1, NSTEP + 1):
            wilson = link_product(wilson, dagger(jnp.roll(link_field, reach, axis=3)))
            results[-reach] = project(colour_apply(wilson, jnp.roll(source, reach, axis=4)))
        return jnp.stack([results[offset] for offset in range(-NSTEP, NSTEP + 1)])
    slices = lax.map(one_slice, (jnp.moveaxis(propagator, 4, 0), jnp.moveaxis(links, 3, 0), cosine_all, sine_all))
    return jnp.take(slices, displacements.astype(jnp.int32), axis=1)
```

```python
import math

import jax
import jax.numpy as jnp
from jax import lax
from jax.experimental import pallas as pl
from jax.experimental.pallas import tpu as pltpu
from jax.sharding import PartitionSpec as P

f32 = jnp.float32
LANES = 128
PAD = 40


def vmem(count):
    return [pl.BlockSpec(memory_space=pltpu.VMEM) for _ in range(count)]


def smem(count):
    return [pl.BlockSpec(memory_space=pltpu.SMEM) for _ in range(count)]


def widen(packed_ref, wide_ref):
    rows = packed_ref.shape[0]
    wide_ref[0:rows, :] = packed_ref[...].astype(f32)
    wide_ref[rows:, :] = jnp.zeros((wide_ref.shape[0] - rows, wide_ref.shape[1]), f32)


def strided(wide_ref, part, spin, first, count, slices, now):
    start = ((part * 36 + first) * slices + now) * 4 + spin
    return wide_ref[pl.ds(start, count, stride=4 * slices), :]


def pair_sums(left_ref, wide_ref, slices, now, keep):
    for u in range(4):
        for s in range(4):
            real = imag = None
            for j in range(PAD // 8):
                rr = strided(wide_ref, 0, u, 8 * j, 8, slices, now)
                ri = strided(wide_ref, 1, u, 8 * j, 8, slices, now)
                lr = left_ref[pl.ds((now * 8 + s) * PAD + 8 * j, 8), :]
                li = left_ref[pl.ds((now * 8 + 4 + s) * PAD + 8 * j, 8), :]
                re = lr * rr - li * ri
                im = lr * ri + li * rr
                real = re if real is None else real + re
                imag = im if imag is None else imag + im
            keep(s, u, real, imag)


def left_rows(left_ref, now, part, s, first, value):
    left_ref[pl.ds((now * 8 + part * 4 + s) * PAD + first, value.shape[0]), :] = value


def dressed(left_ref, wide_ref, wilson, slices, now):
    zeros = jnp.zeros((PAD - 36, left_ref.shape[1]), f32)
    for s in range(4):
        for b in range(3):
            real = imag = None
            for a in range(3):
                sr = strided(wide_ref, 0, s, a * 12, 12, slices, now)
                si = strided(wide_ref, 1, s, a * 12, 12, slices, now)
                wr, wi = wilson(0, a, b), wilson(1, a, b)
                re = sr * wr + si * wi
                im = sr * wi - si * wr
                real = re if real is None else real + re
                imag = im if imag is None else imag + im
            left_rows(left_ref, now, 0, s, b * 12, real)
            left_rows(left_ref, now, 1, s, b * 12, imag)
        left_rows(left_ref, now, 0, s, 36, zeros)
        left_rows(left_ref, now, 1, s, 36, zeros)


def pairs_at(ref, now, s, u):
    base = now * 256 + (s * 4 + u) * 8
    return ref[pl.ds(pl.multiple_of(base, 8), 8), :], ref[pl.ds(pl.multiple_of(base + 128, 8), 8), :]


def keeper(ref, now):
    def keep(s, u, real, imag):
        ref[pl.ds(now * 256 + (s * 4 + u) * 8, 8), :] = real
        ref[pl.ds(now * 256 + 128 + (s * 4 + u) * 8, 8), :] = imag

    return keep


def first_kernel(slices, source_ref, links_ref, left_ref, pairs_ref, wilson_ref, wide_ref, plain_ref):
    widen(source_ref, wide_ref)
    for now in range(slices):
        zeros = jnp.zeros((PAD - 36, left_ref.shape[1]), f32)
        for s in range(4):
            left_rows(plain_ref, now, 0, s, 0, strided(wide_ref, 0, s, 0, 36, slices, now))
            left_rows(plain_ref, now, 1, s, 0, -strided(wide_ref, 1, s, 0, 36, slices, now))
            left_rows(plain_ref, now, 0, s, 36, zeros)
            left_rows(plain_ref, now, 1, s, 36, zeros)
        pair_sums(plain_ref, wide_ref, slices, now, keeper(pairs_ref, now))
        for part in range(2):
            for a in range(3):
                for b in range(3):
                    wilson_ref[pl.ds((now * 2 + part) * 9 + a * 3 + b, 1), :] = links_ref[a, b, now, part : part + 1, :].astype(f32)
        dressed(left_ref, wide_ref, lambda part, a, b: wilson_ref[pl.ds((now * 2 + part) * 9 + a * 3 + b, 1), :], slices, now)


def further_kernel(slices, source_ref, moved_ref, before_ref, left_ref, wilson_ref, wide_ref):
    widen(source_ref, wide_ref)
    for now in range(slices):
        def link(part, a, b):
            return moved_ref[a, b, now, part : part + 1, :].astype(f32)

        def old(part, a, b):
            return before_ref[pl.ds((now * 2 + part) * 9 + a * 3 + b, 1), :]

        for a in range(3):
            for b in range(3):
                real = sum(old(0, a, m) * link(0, m, b) - old(1, a, m) * link(1, m, b) for m in range(3))
                imag = sum(old(0, a, m) * link(1, m, b) + old(1, a, m) * link(0, m, b) for m in range(3))
                wilson_ref[pl.ds(now * 18 + a * 3 + b, 1), :] = real
                wilson_ref[pl.ds(now * 18 + 9 + a * 3 + b, 1), :] = imag
        dressed(left_ref, wide_ref, lambda part, a, b: wilson_ref[pl.ds((now * 2 + part) * 9 + a * 3 + b, 1), :], slices, now)


def pairs_kernel(slices, left_ref, moved_ref, pairs_ref, wide_ref):
    widen(moved_ref, wide_ref)
    for now in range(slices):
        pair_sums(left_ref, wide_ref, slices, now, keeper(pairs_ref, now))


def gamma_traces(pairs_ref, now, perm_ref, turn_ref, g, mirrored):
    real = imag = None
    for s in range(4):
        u = perm_ref[g, s]
        pr, pi = pairs_at(pairs_ref, now, u, s) if mirrored else pairs_at(pairs_ref, now, s, u)
        if mirrored:
            pi = -pi
        turn = turn_ref[g, s]
        cr = jnp.where(turn == 0, 1.0, jnp.where(turn == 2, -1.0, 0.0)).astype(f32)
        ci = jnp.where(turn == 1, 1.0, jnp.where(turn == 3, -1.0, 0.0)).astype(f32)
        re = cr * pr - ci * pi
        im = cr * pi + ci * pr
        real = re if real is None else real + re
        imag = im if imag is None else imag + im
    return jnp.sum(real, axis=0, keepdims=True), jnp.sum(imag, axis=0, keepdims=True)


def last_kernel(slices, nsteps, perm_ref, turn_ref, place_ref, left_ref, moved_ref, tables_ref, *rest):
    earlier, (out_ref, wide_ref, pairs_ref, real_ref, imag_ref) = rest[:nsteps], rest[nsteps:]
    widen(moved_ref, wide_ref)
    total = None
    rows = real_ref.shape[0]
    for now in range(slices):
        pair_sums(left_ref, wide_ref, slices, now, keeper(pairs_ref, now))
        real_ref[...] = jnp.zeros_like(real_ref)
        imag_ref[...] = jnp.zeros_like(imag_ref)
        for reach in range(nsteps + 1):
            source = pairs_ref if reach == nsteps else earlier[reach]
            for sign in (1, -1) if reach else (1,):
                for g in range(4):
                    re, im = gamma_traces(source, now, perm_ref, turn_ref, g, sign < 0)
                    row = place_ref[nsteps + sign * reach] * 4 + g
                    real_ref[pl.ds(row, 1), :] = re
                    imag_ref[pl.ds(row, 1), :] = im
        re = jnp.sum(real_ref[...], axis=1, keepdims=True)
        im = jnp.sum(imag_ref[...], axis=1, keepdims=True)
        part = re * tables_ref[now, 0] + im * tables_ref[now, 1]
        total = part if total is None else total + part
    out_ref[...] = total


def final_kernel(slices_all, entries, mine_ref, other_ref, out_ref):
    total = mine_ref[...] + other_ref[...]
    for t in range(slices_all):
        for c in range(2):
            for row in range(entries):
                at = t * 8 + c * 4
                out_ref[t, row // 4, row % 4, c : c + 1, :] = total[row : row + 1, at : at + 4]


def from_behind(array, axis, by):
    peers = lax.axis_size(axis)
    return lax.ppermute(array, axis, [(i, (i + by) % peers) for i in range(peers)])


def swap(array, mapping, sizes, axes):
    nt, nz, ny = sizes
    pairs = []
    for t in range(nt):
        for z in range(nz):
            for y in range(ny):
                a, b, c = mapping(t, z, y)
                pairs.append(((t * nz + z) * ny + y, (a * nz + b) * ny + c))
    return lax.ppermute(array, axes, pairs)


def body(propagator, links, source_z, displacements, momenta, gamma_perm, gamma_phase):
    axes = ("ta", "gz", "gy")
    sizes = tuple(lax.axis_size(a) for a in axes)
    depth_count = sizes[1]
    entries = displacements.shape[0]
    nsteps = (entries - 1) // 2
    slices = propagator.shape[4]
    sites = propagator.shape[6]
    slices_all = slices * sizes[0]
    scaling = 1.0 / (24.0 * math.sqrt(sites * sizes[2] * depth_count))
    source = jnp.reshape(jnp.transpose(propagator, (0, 2, 3, 4, 5, 1, 6)), (288 * slices, sites))
    linked = jnp.reshape(jnp.transpose(links, (1, 2, 3, 4, 0, 5)), (3, 3, slices, 2, sites))
    moved, moved_links = source, linked
    wide = pltpu.VMEM((288 * slices + 16 * slices, sites), f32)
    rows = -(-entries * 4 // 8) * 8

    depth = lax.axis_index("gz")
    first_slice = lax.axis_index("ta") * slices
    lane = jnp.arange(LANES, dtype=jnp.int32)
    lane_slice, lane_part, lane_p = lane // 8, (lane // 4) % 2, lane % 4
    hot_p = (lane_p[:, None] == jnp.arange(4)[None, :]).astype(jnp.int32)
    lane_mom = jnp.sum(hot_p * momenta[None, :], axis=1)
    hot_t = (lane_slice[:, None] == jnp.arange(slices_all)[None, :]).astype(jnp.int32)
    lane_src = jnp.sum(hot_t[:, :, None] * hot_p[:, None, :] * source_z[None, :, :], axis=(1, 2))
    row_entry = jnp.arange(rows, dtype=jnp.int32) // 4
    offset = jnp.sum((row_entry[:, None] == jnp.arange(entries)[None, :]).astype(jnp.int32) * displacements[None, :], axis=1) - nsteps
    ahead = jnp.maximum(-offset, 0)
    turn = lane_mom[None, :] * (depth + ahead[:, None] - lane_src[None, :]) % depth_count
    angle = turn.astype(f32) * (2.0 * math.pi / depth_count)
    cosine, sine = jnp.cos(angle) * scaling, jnp.sin(angle) * scaling
    first = jnp.where(lane_part == 0, cosine, -sine)
    second = jnp.where(lane_part == 0, sine, cosine)
    own = (lane_slice[None, :] == first_slice + jnp.arange(slices)[:, None]).astype(f32)
    tables = own[:, None, None, :] * jnp.stack([first, second])[None]
    place = jnp.sum((displacements[None, :] == jnp.arange(entries)[:, None]) * jnp.arange(entries, dtype=jnp.int32)[None, :], axis=1).astype(jnp.int32)

    moved = from_behind(moved, "gz", -1)
    shape_left = jax.ShapeDtypeStruct((slices * 8 * PAD, sites), f32)
    shape_pairs = jax.ShapeDtypeStruct((slices * 256, sites), f32)
    shape_wilson = jax.ShapeDtypeStruct((slices * 18, sites), f32)
    left, pairs, wilson = pl.pallas_call(
        lambda *refs: first_kernel(slices, *refs),
        out_shape=(shape_left, shape_pairs, shape_wilson),
        in_specs=vmem(2),
        out_specs=tuple(vmem(3)),
        scratch_shapes=[wide, pltpu.VMEM((slices * 8 * PAD, sites), f32)],
        name="local",
    )(source, linked)
    earlier = [pairs]
    for reach in range(1, nsteps):
        earlier.append(
            pl.pallas_call(
                lambda *refs: pairs_kernel(slices, *refs),
                out_shape=shape_pairs,
                in_specs=vmem(2),
                out_specs=vmem(1)[0],
                scratch_shapes=[wide],
                name="pairs",
            )(left, moved)
        )
        moved_links = from_behind(moved_links, "gz", -1)
        moved = from_behind(moved, "gz", -1)
        left, wilson = pl.pallas_call(
            lambda *refs: further_kernel(slices, *refs),
            out_shape=(shape_left, shape_wilson),
            in_specs=vmem(3),
            out_specs=tuple(vmem(2)),
            scratch_shapes=[wide],
            name="further",
        )(source, moved_links, wilson)
    total = pl.pallas_call(
        lambda *refs: last_kernel(slices, nsteps, *refs),
        out_shape=jax.ShapeDtypeStruct((rows, LANES), f32),
        in_specs=smem(3) + vmem(3 + nsteps),
        out_specs=vmem(1)[0],
        scratch_shapes=[wide, pltpu.VMEM((slices * 256, sites), f32), pltpu.VMEM((rows, sites), f32), pltpu.VMEM((rows, sites), f32)],
        name="last",
    )(gamma_perm, gamma_phase, place, left, moved, tables, *earlier)

    moves = []
    bit = 1
    while bit < sizes[1]:
        moves.append((0, bit, 0) if bit == 1 else (0, bit + 1, 0))
        bit *= 2
    for axis, size in ((0, sizes[0]), (2, sizes[2])):
        bit = 1
        while bit < size:
            moves.append(tuple(bit if a == axis else (1 if a == 1 else 0) for a in range(3)))
            bit *= 2
    received = None
    for t_bits, z_bits, y_bits in moves:
        if received is not None:
            total = total + received
        received = swap(total, lambda t, z, y: (t ^ t_bits, z ^ z_bits, y ^ y_bits), sizes, axes)
    out = pl.pallas_call(
        lambda *refs: final_kernel(slices_all, entries * 4, *refs),
        out_shape=jax.ShapeDtypeStruct((slices_all, entries, 4, 2, 4), f32),
        in_specs=vmem(2),
        name="final",
    )(total, received)
    return jnp.transpose(out, (0, 1, 2, 4, 3))


def solution(mesh):
    placed = (
        P(None, None, None, None, "ta", "gz", "gy"),
        P(None, None, None, "ta", "gz", "gy"),
        P(),
        P(),
        P(),
        P(),
        P(),
    )
    return jax.shard_map(body, mesh=mesh, in_specs=placed, out_specs=P(), check_vma=False)
```

```python
import math

import jax
import jax.numpy as jnp
from jax import lax
from jax.experimental import pallas as pl
from jax.experimental.pallas import tpu as pltpu
from jax.sharding import PartitionSpec as P

f32 = jnp.float32
LANES = 128
PAD = 40


def vmem(count):
    return [pl.BlockSpec(memory_space=pltpu.VMEM) for _ in range(count)]


def near(array):
    return pltpu.with_memory_space_constraint(array, pltpu.VMEM)


def kept(shape):
    return pltpu.VMEM(shape, f32)


def smem(count):
    return [pl.BlockSpec(memory_space=pltpu.SMEM) for _ in range(count)]


def widen(packed_ref, wide_ref):
    rows = packed_ref.shape[0]
    wide_ref[0:rows, :] = packed_ref[...].astype(f32)
    wide_ref[rows:, :] = jnp.zeros((wide_ref.shape[0] - rows, wide_ref.shape[1]), f32)


def strided(wide_ref, part, spin, first, count, slices, now):
    start = ((part * 36 + first) * slices + now) * 4 + spin
    return wide_ref[pl.ds(start, count, stride=4 * slices), :]


def pair_sums(left_ref, wide_ref, slices, now, keep):
    for u in range(4):
        for s in range(4):
            real = imag = None
            for j in range(PAD // 8):
                rr = strided(wide_ref, 0, u, 8 * j, 8, slices, now)
                ri = strided(wide_ref, 1, u, 8 * j, 8, slices, now)
                lr = left_ref[pl.ds((now * 8 + s) * PAD + 8 * j, 8), :]
                li = left_ref[pl.ds((now * 8 + 4 + s) * PAD + 8 * j, 8), :]
                re = lr * rr - li * ri
                im = lr * ri + li * rr
                real = re if real is None else real + re
                imag = im if imag is None else imag + im
            keep(s, u, real, imag)


def left_rows(left_ref, now, part, s, first, value):
    left_ref[pl.ds((now * 8 + part * 4 + s) * PAD + first, value.shape[0]), :] = value


def dressed(left_ref, wide_ref, wilson, slices, now):
    zeros = jnp.zeros((PAD - 36, left_ref.shape[1]), f32)
    for s in range(4):
        for b in range(3):
            real = imag = None
            for a in range(3):
                sr = strided(wide_ref, 0, s, a * 12, 12, slices, now)
                si = strided(wide_ref, 1, s, a * 12, 12, slices, now)
                wr, wi = wilson(0, a, b), wilson(1, a, b)
                re = sr * wr + si * wi
                im = sr * wi - si * wr
                real = re if real is None else real + re
                imag = im if imag is None else imag + im
            left_rows(left_ref, now, 0, s, b * 12, real)
            left_rows(left_ref, now, 1, s, b * 12, imag)
        left_rows(left_ref, now, 0, s, 36, zeros)
        left_rows(left_ref, now, 1, s, 36, zeros)


def keep_pairs(ref, now):
    def keep(s, u, real, imag):
        ref[pl.ds((s * 4 + u) * 8, 8), :] = real
        ref[pl.ds(128 + (s * 4 + u) * 8, 8), :] = imag

    return keep


def power_of_i(turn):
    real = jnp.where(turn == 0, 1.0, jnp.where(turn == 2, -1.0, 0.0)).astype(f32)
    imag = jnp.where(turn == 1, 1.0, jnp.where(turn == 3, -1.0, 0.0)).astype(f32)
    return real, imag


def tile_at(first):
    return pl.ds(first if isinstance(first, int) else pl.multiple_of(first, 8), 8)


def insert(plain_ref, left_ref, perm_ref, turn_ref, now):
    for g in range(4):
        for s in range(4):
            u = perm_ref[g, s]
            cr, ci = power_of_i(turn_ref[g, s])
            for mirrored in range(2):
                base = (now * 2 + mirrored) * 8 + g * 2
                taken, put, sign = (u, s, -1.0) if mirrored else (s, u, 1.0)
                for j in range(PAD // 8):
                    lr = plain_ref[tile_at((now * 8 + taken) * PAD + 8 * j), :]
                    li = plain_ref[tile_at((now * 8 + 4 + taken) * PAD + 8 * j), :]
                    left_ref[tile_at((base * 4 + put) * PAD + 8 * j), :] = cr * lr - (sign * ci) * li
                    left_ref[tile_at((base * 4 + 4 + put) * PAD + 8 * j), :] = cr * li + (sign * ci) * lr


def meet(left_ref, wide_ref, slices, now, rows_ref, first):
    sums = [None] * 16
    for u in range(4):
        for j in range(PAD // 8):
            rr = strided(wide_ref, 0, u, 8 * j, 8, slices, now)
            ri = strided(wide_ref, 1, u, 8 * j, 8, slices, now)
            for which in range(8):
                base = ((now * 16 + which * 2) * 4 + u) * PAD + 8 * j
                lr = left_ref[pl.ds(base, 8), :]
                li = left_ref[pl.ds(base + 4 * PAD, 8), :]
                re = lr * rr - li * ri
                im = lr * ri + li * rr
                at = (which // 4) * 8 + which % 4
                sums[at] = re if sums[at] is None else sums[at] + re
                sums[at + 4] = im if sums[at + 4] is None else sums[at + 4] + im
    for at in range(16):
        rows_ref[pl.ds(first + at, 1), :] = jnp.sum(sums[at], axis=0, keepdims=True)


def fill_tables(tables_ref, sizes, scaling, slices, entries, source_ref, entry_ref, momenta_ref):
    slices_all, depth_count = sizes
    nsteps = (entries - 1) // 2
    rows = tables_ref.shape[1]
    depth, first_slice = lax.axis_index("gz"), lax.axis_index("ta") * slices
    lane = lax.broadcasted_iota(jnp.int32, (8, LANES), 1)
    lane_slice, lane_part, lane_p = lane // 8, (lane // 4) % 2, lane % 4
    momentum = jnp.zeros((8, LANES), jnp.int32)
    origin = jnp.zeros((8, LANES), jnp.int32)
    for p in range(4):
        momentum = jnp.where(lane_p == p, momenta_ref[p], momentum)
        for t in range(slices_all):
            origin = jnp.where((lane_p == p) & (lane_slice == t), source_ref[t, p], origin)
    row = lax.broadcasted_iota(jnp.int32, (rows, LANES), 0)
    for l in range(entries):
        ahead = max(nsteps - l, 0)
        turn = lax.rem(momentum * (depth + ahead + depth_count - origin), depth_count)
        angle = turn.astype(f32) * (2.0 * math.pi / depth_count)
        cosine, sine = jnp.cos(angle) * scaling, jnp.sin(angle) * scaling
        first = jnp.where(lane_part == 0, cosine, -sine)
        second = jnp.where(lane_part == 0, sine, cosine)
        if l < nsteps:
            second = -second
        place = sum(jnp.where(entry_ref[j] == l, j, 0) for j in range(entries))
        for now in range(slices):
            own = lane_slice == first_slice + now
            for g in range(4):
                hit = row == place * 4 + g
                for which, table in ((0, first), (1, second)):
                    mine = jnp.where(own, table, 0.0)[0:1, :]
                    tables_ref[((now * entries + l) * 4 + g) * 2 + which] = jnp.where(hit, mine, 0.0)


def first_kernel(slices, sizes, scaling, entries, source_z_ref, entry_ref, momenta_ref, perm_ref, turn_ref, source_ref, links_ref,
                 left_ref, rows_ref, tables_ref, wilson_ref, wide_ref, plain_ref, pairs_ref):
    widen(source_ref, wide_ref)
    fill_tables(tables_ref, sizes, scaling, slices, entries, source_z_ref, entry_ref, momenta_ref)
    zeros = jnp.zeros((PAD - 36, LANES), f32)
    for now in range(slices):
        for s in range(4):
            left_rows(plain_ref, now, 0, s, 0, strided(wide_ref, 0, s, 0, 36, slices, now))
            left_rows(plain_ref, now, 1, s, 0, -strided(wide_ref, 1, s, 0, 36, slices, now))
            left_rows(plain_ref, now, 0, s, 36, zeros)
            left_rows(plain_ref, now, 1, s, 36, zeros)
        pair_sums(plain_ref, wide_ref, slices, now, keep_pairs(pairs_ref, now))
        for g in range(4):
            real = imag = None
            for s in range(4):
                at = (s * 4 + perm_ref[g, s]) * 8
                pr, pi = pairs_ref[tile_at(at), :], pairs_ref[tile_at(at + 128), :]
                cr, ci = power_of_i(turn_ref[g, s])
                re, im = cr * pr - ci * pi, cr * pi + ci * pr
                real = re if real is None else real + re
                imag = im if imag is None else imag + im
            rows_ref[now * 8 + g : now * 8 + g + 1, :] = jnp.sum(real, axis=0, keepdims=True)
            rows_ref[now * 8 + 4 + g : now * 8 + 5 + g, :] = jnp.sum(imag, axis=0, keepdims=True)
        for part in range(2):
            for a in range(3):
                for b in range(3):
                    wilson_ref[pl.ds((now * 2 + part) * 9 + a * 3 + b, 1), :] = links_ref[a, b, now, part : part + 1, :].astype(f32)
        dressed(plain_ref, wide_ref, lambda part, a, b: wilson_ref[pl.ds((now * 2 + part) * 9 + a * 3 + b, 1), :], slices, now)
        insert(plain_ref, left_ref, perm_ref, turn_ref, now)


def further_kernel(slices, perm_ref, turn_ref, source_ref, moved_ref, before_ref, left_ref, wilson_ref, wide_ref, plain_ref):
    widen(source_ref, wide_ref)
    for now in range(slices):
        def link(part, a, b):
            return moved_ref[a, b, now, part : part + 1, :].astype(f32)

        def old(part, a, b):
            return before_ref[pl.ds((now * 2 + part) * 9 + a * 3 + b, 1), :]

        for a in range(3):
            for b in range(3):
                real = sum(old(0, a, m) * link(0, m, b) - old(1, a, m) * link(1, m, b) for m in range(3))
                imag = sum(old(0, a, m) * link(1, m, b) + old(1, a, m) * link(0, m, b) for m in range(3))
                wilson_ref[pl.ds(now * 18 + a * 3 + b, 1), :] = real
                wilson_ref[pl.ds(now * 18 + 9 + a * 3 + b, 1), :] = imag
        dressed(plain_ref, wide_ref, lambda part, a, b: wilson_ref[pl.ds((now * 2 + part) * 9 + a * 3 + b, 1), :], slices, now)
        insert(plain_ref, left_ref, perm_ref, turn_ref, now)


def middle_kernel(slices, left_ref, moved_ref, rows_ref, wide_ref):
    widen(moved_ref, wide_ref)
    for now in range(slices):
        meet(left_ref, wide_ref, slices, now, rows_ref, now * 16)


def last_kernel(slices, nsteps, left_ref, moved_ref, tables_ref, *rest):
    earlier, (out_ref, wide_ref, rows_ref) = rest[:nsteps], rest[nsteps:]
    widen(moved_ref, wide_ref)
    total = None
    entries = 2 * nsteps + 1
    for now in range(slices):
        rows_ref[nsteps * 8 : nsteps * 8 + 8, :] = earlier[0][now * 8 : now * 8 + 8, :]
        for reach in range(1, nsteps):
            rows_ref[(nsteps + reach) * 8 : (nsteps + reach) * 8 + 8, :] = earlier[reach][now * 16 : now * 16 + 8, :]
            rows_ref[(nsteps - reach) * 8 : (nsteps - reach) * 8 + 8, :] = earlier[reach][now * 16 + 8 : now * 16 + 16, :]
        meet(left_ref, wide_ref, slices, now, rows_ref, entries * 8)
        rows_ref[2 * nsteps * 8 : entries * 8, :] = rows_ref[entries * 8 : entries * 8 + 8, :]
        rows_ref[0:8, :] = rows_ref[entries * 8 + 8 : entries * 8 + 16, :]
        summed = jnp.sum(rows_ref[0 : entries * 8, :], axis=1, keepdims=True)
        rows_ref[0 : entries * 8, :] = jnp.broadcast_to(summed, (entries * 8, LANES))
        for l in range(entries):
            for g in range(4):
                at = ((now * entries + l) * 4 + g) * 2
                part = rows_ref[l * 8 + g : l * 8 + g + 1, :] * tables_ref[at] + rows_ref[l * 8 + 4 + g : l * 8 + 5 + g, :] * tables_ref[at + 1]
                total = part if total is None else total + part
    out_ref[...] = total


def final_kernel(slices_all, entries, mine_ref, other_ref, out_ref):
    total = mine_ref[...] + other_ref[...]
    for t in range(slices_all):
        for c in range(2):
            for row in range(entries):
                at = t * 8 + c * 4
                out_ref[t, row // 4, row % 4, c : c + 1, :] = total[row : row + 1, at : at + 4]


def from_behind(array, axis, by):
    peers = lax.axis_size(axis)
    return lax.ppermute(array, axis, [(i, (i + by) % peers) for i in range(peers)])


def swap(array, mapping, sizes, axes):
    nt, nz, ny = sizes
    pairs = []
    for t in range(nt):
        for z in range(nz):
            for y in range(ny):
                a, b, c = mapping(t, z, y)
                pairs.append(((t * nz + z) * ny + y, (a * nz + b) * ny + c))
    return lax.ppermute(array, axes, pairs)


def body(propagator, links, source_z, displacements, momenta, gamma_perm, gamma_phase):
    axes = ("ta", "gz", "gy")
    sizes = tuple(lax.axis_size(a) for a in axes)
    depth_count = sizes[1]
    entries = displacements.shape[0]
    nsteps = (entries - 1) // 2
    slices = propagator.shape[4]
    sites = propagator.shape[6]
    slices_all = slices * sizes[0]
    scaling = 1.0 / (24.0 * math.sqrt(sites * sizes[2] * depth_count))
    source = jnp.reshape(jnp.transpose(propagator, (0, 2, 3, 4, 5, 1, 6)), (288 * slices, sites))
    linked = jnp.reshape(jnp.transpose(links, (1, 2, 3, 4, 0, 5)), (3, 3, slices, 2, sites))
    moved, moved_links = source, linked
    wide = pltpu.VMEM((288 * slices + 16 * slices, sites), f32)
    plain = pltpu.VMEM((slices * 8 * PAD, sites), f32)
    rows = -(-entries * 4 // 8) * 8

    moved = from_behind(moved, "gz", -1)
    shape_left = kept((slices * 64 * PAD, sites))
    shape_wilson = kept((slices * 18, sites))
    left, first_rows, tables, wilson = pl.pallas_call(
        lambda *refs: first_kernel(slices, (slices_all, depth_count), scaling, entries, *refs),
        out_shape=(shape_left, kept((slices * 8, sites)), kept((slices * entries * 8, rows, LANES)), shape_wilson),
        in_specs=smem(5) + vmem(2),
        out_specs=tuple(vmem(4)),
        scratch_shapes=[wide, plain, pltpu.VMEM((256, sites), f32)],
        name="local",
    )(source_z, displacements, momenta, gamma_perm, gamma_phase, source, linked)
    earlier = [first_rows]
    for reach in range(1, nsteps):
        earlier.append(
            pl.pallas_call(
                lambda *refs: middle_kernel(slices, *refs),
                out_shape=kept((slices * 16, sites)),
                in_specs=vmem(2),
                out_specs=vmem(1)[0],
                scratch_shapes=[wide],
                name="middle",
            )(near(left), near(moved))
        )
        moved_links = from_behind(moved_links, "gz", -1)
        moved = from_behind(moved, "gz", -1)
        left, wilson = pl.pallas_call(
            lambda *refs: further_kernel(slices, *refs),
            out_shape=(shape_left, shape_wilson),
            in_specs=smem(2) + vmem(3),
            out_specs=tuple(vmem(2)),
            scratch_shapes=[wide, plain],
            name="further",
        )(gamma_perm, gamma_phase, source, moved_links, near(wilson))
    total = pl.pallas_call(
        lambda *refs: last_kernel(slices, nsteps, *refs),
        out_shape=kept((rows, LANES)),
        in_specs=vmem(3 + nsteps),
        out_specs=vmem(1)[0],
        scratch_shapes=[wide, pltpu.VMEM((entries * 8 + 16, sites), f32)],
        name="last",
    )(near(left), near(moved), near(tables), *(near(e) for e in earlier))

    moves = []
    bit = 1
    while bit < sizes[1]:
        moves.append((0, bit, 0) if bit == 1 else (0, bit + 1, 0))
        bit *= 2
    for axis, size in ((0, sizes[0]), (2, sizes[2])):
        bit = 1
        while bit < size:
            moves.append(tuple(bit if a == axis else (1 if a == 1 else 0) for a in range(3)))
            bit *= 2
    received = None
    for t_bits, z_bits, y_bits in moves:
        if received is not None:
            total = total + received
        received = swap(total, lambda t, z, y: (t ^ t_bits, z ^ z_bits, y ^ y_bits), sizes, axes)
    out = pl.pallas_call(
        lambda *refs: final_kernel(slices_all, entries * 4, *refs),
        out_shape=jax.ShapeDtypeStruct((slices_all, entries, 4, 2, 4), f32),
        in_specs=vmem(2),
        name="final",
    )(near(total), near(received))
    return jnp.transpose(out, (0, 1, 2, 4, 3))


def solution(mesh):
    placed = (
        P(None, None, None, None, "ta", "gz", "gy"),
        P(None, None, None, "ta", "gz", "gy"),
        P(),
        P(),
        P(),
        P(),
        P(),
    )
    return jax.shard_map(body, mesh=mesh, in_specs=placed, out_specs=P(), check_vma=False)
```

```python
import math

import jax
import jax.numpy as jnp
from jax import lax
from jax.experimental import pallas as pl
from jax.experimental.pallas import tpu as pltpu
from jax.sharding import PartitionSpec as P

f32 = jnp.float32
LANES = 128
PAD = 40


def vmem(count):
    return [pl.BlockSpec(memory_space=pltpu.VMEM) for _ in range(count)]


def near(array):
    return pltpu.with_memory_space_constraint(array, pltpu.VMEM)


def kept(shape):
    return pltpu.VMEM(shape, f32)


def smem(count):
    return [pl.BlockSpec(memory_space=pltpu.SMEM) for _ in range(count)]


def widen(packed_ref, wide_ref):
    rows = packed_ref.shape[0]
    wide_ref[0:rows, :] = packed_ref[...].astype(f32)
    wide_ref[rows:, :] = jnp.zeros((wide_ref.shape[0] - rows, wide_ref.shape[1]), f32)


def strided(wide_ref, part, spin, first, count, slices, now):
    start = ((part * 36 + first) * slices + now) * 4 + spin
    return wide_ref[pl.ds(start, count, stride=4 * slices), :]


def pair_sums(left_ref, wide_ref, slices, now, keep):
    for u in range(4):
        for s in range(4):
            real = imag = None
            for j in range(PAD // 8):
                rr = strided(wide_ref, 0, u, 8 * j, 8, slices, now)
                ri = strided(wide_ref, 1, u, 8 * j, 8, slices, now)
                lr = left_ref[pl.ds((now * 8 + s) * PAD + 8 * j, 8), :]
                li = left_ref[pl.ds((now * 8 + 4 + s) * PAD + 8 * j, 8), :]
                re = lr * rr - li * ri
                im = lr * ri + li * rr
                real = re if real is None else real + re
                imag = im if imag is None else imag + im
            keep(s, u, real, imag)


def left_rows(left_ref, now, part, s, first, value):
    left_ref[pl.ds((now * 8 + part * 4 + s) * PAD + first, value.shape[0]), :] = value


def dressed(left_ref, wide_ref, wilson, slices, now):
    zeros = jnp.zeros((PAD - 36, left_ref.shape[1]), f32)
    for s in range(4):
        for b in range(3):
            real = imag = None
            for a in range(3):
                sr = strided(wide_ref, 0, s, a * 12, 12, slices, now)
                si = strided(wide_ref, 1, s, a * 12, 12, slices, now)
                wr, wi = wilson(0, a, b), wilson(1, a, b)
                re = sr * wr + si * wi
                im = sr * wi - si * wr
                real = re if real is None else real + re
                imag = im if imag is None else imag + im
            left_rows(left_ref, now, 0, s, b * 12, real)
            left_rows(left_ref, now, 1, s, b * 12, imag)
        left_rows(left_ref, now, 0, s, 36, zeros)
        left_rows(left_ref, now, 1, s, 36, zeros)


def keep_pairs(ref, now):
    def keep(s, u, real, imag):
        ref[pl.ds((s * 4 + u) * 8, 8), :] = real
        ref[pl.ds(128 + (s * 4 + u) * 8, 8), :] = imag

    return keep


def power_of_i(turn):
    real = jnp.where(turn == 0, 1.0, jnp.where(turn == 2, -1.0, 0.0)).astype(f32)
    imag = jnp.where(turn == 1, 1.0, jnp.where(turn == 3, -1.0, 0.0)).astype(f32)
    return real, imag


def tile_at(first):
    return pl.ds(first if isinstance(first, int) else pl.multiple_of(first, 8), 8)


def insert(plain_ref, left_ref, perm_ref, turn_ref, now):
    for g in range(4):
        for s in range(4):
            u = perm_ref[g, s]
            cr, ci = power_of_i(turn_ref[g, s])
            for mirrored in range(2):
                base = (now * 2 + mirrored) * 8 + g * 2
                taken, put, sign = (u, s, -1.0) if mirrored else (s, u, 1.0)
                for j in range(PAD // 8):
                    lr = plain_ref[tile_at((now * 8 + taken) * PAD + 8 * j), :]
                    li = plain_ref[tile_at((now * 8 + 4 + taken) * PAD + 8 * j), :]
                    left_ref[tile_at((base * 4 + put) * PAD + 8 * j), :] = cr * lr - (sign * ci) * li
                    left_ref[tile_at((base * 4 + 4 + put) * PAD + 8 * j), :] = cr * li + (sign * ci) * lr


def meet(left_ref, wide_ref, slices, now, rows_ref, first):
    sums = [None] * 16
    for u in range(4):
        for j in range(PAD // 8):
            rr = strided(wide_ref, 0, u, 8 * j, 8, slices, now)
            ri = strided(wide_ref, 1, u, 8 * j, 8, slices, now)
            for which in range(8):
                base = ((now * 16 + which * 2) * 4 + u) * PAD + 8 * j
                lr = left_ref[pl.ds(base, 8), :]
                li = left_ref[pl.ds(base + 4 * PAD, 8), :]
                re = lr * rr - li * ri
                im = lr * ri + li * rr
                at = (which // 4) * 8 + which % 4
                sums[at] = re if sums[at] is None else sums[at] + re
                sums[at + 4] = im if sums[at + 4] is None else sums[at + 4] + im
    for at in range(16):
        rows_ref[pl.ds(first + at, 1), :] = jnp.sum(sums[at], axis=0, keepdims=True)


def fill_tables(tables_ref, sizes, scaling, slices, entries, source_ref, entry_ref, momenta_ref):
    slices_all, depth_count = sizes
    nsteps = (entries - 1) // 2
    rows = tables_ref.shape[1]
    depth, first_slice = lax.axis_index("gz"), lax.axis_index("ta") * slices
    lane = lax.broadcasted_iota(jnp.int32, (rows, LANES), 1)
    slot = lax.broadcasted_iota(jnp.int32, (rows, LANES), 0) * (LANES // 8) + lane // 8
    lane_part, lane_p = (lane // 4) % 2, lane % 4
    momentum = jnp.zeros((rows, LANES), jnp.int32)
    for p in range(4):
        momentum = jnp.where(lane_p == p, momenta_ref[p], momentum)
    for now in range(slices):
        origin = jnp.zeros((rows, LANES), jnp.int32)
        for p in range(4):
            origin = jnp.where(lane_p == p, source_ref[first_slice + now, p], origin)
        for l in range(entries):
            ahead = max(nsteps - l, 0)
            turn = lax.rem(momentum * (depth + ahead + depth_count - origin), depth_count)
            angle = turn.astype(f32) * (2.0 * math.pi / depth_count)
            cosine, sine = jnp.cos(angle) * scaling, jnp.sin(angle) * scaling
            first = jnp.where(lane_part == 0, cosine, -sine)
            second = jnp.where(lane_part == 0, sine, cosine)
            if l < nsteps:
                second = -second
            place = sum(jnp.where(entry_ref[j] == l, j, 0) for j in range(entries))
            for g in range(4):
                at = ((now * entries + l) * 4 + g) * 2
                tables_ref[at] = jnp.where(slot == place * 4 + g, first, 0.0)
                tables_ref[at + 1] = jnp.where(slot == place * 4 + g, second, 0.0)


def first_kernel(slices, sizes, scaling, entries, source_z_ref, entry_ref, momenta_ref, perm_ref, turn_ref, source_ref, links_ref,
                 left_ref, rows_ref, tables_ref, wilson_ref, wide_ref, plain_ref, pairs_ref):
    widen(source_ref, wide_ref)
    fill_tables(tables_ref, sizes, scaling, slices, entries, source_z_ref, entry_ref, momenta_ref)
    zeros = jnp.zeros((PAD - 36, LANES), f32)
    for now in range(slices):
        for s in range(4):
            left_rows(plain_ref, now, 0, s, 0, strided(wide_ref, 0, s, 0, 36, slices, now))
            left_rows(plain_ref, now, 1, s, 0, -strided(wide_ref, 1, s, 0, 36, slices, now))
            left_rows(plain_ref, now, 0, s, 36, zeros)
            left_rows(plain_ref, now, 1, s, 36, zeros)
        pair_sums(plain_ref, wide_ref, slices, now, keep_pairs(pairs_ref, now))
        for g in range(4):
            real = imag = None
            for s in range(4):
                at = (s * 4 + perm_ref[g, s]) * 8
                pr, pi = pairs_ref[tile_at(at), :], pairs_ref[tile_at(at + 128), :]
                cr, ci = power_of_i(turn_ref[g, s])
                re, im = cr * pr - ci * pi, cr * pi + ci * pr
                real = re if real is None else real + re
                imag = im if imag is None else imag + im
            rows_ref[now * 8 + g : now * 8 + g + 1, :] = jnp.sum(real, axis=0, keepdims=True)
            rows_ref[now * 8 + 4 + g : now * 8 + 5 + g, :] = jnp.sum(imag, axis=0, keepdims=True)
        for part in range(2):
            for a in range(3):
                for b in range(3):
                    wilson_ref[pl.ds((now * 2 + part) * 9 + a * 3 + b, 1), :] = links_ref[a, b, now, part : part + 1, :].astype(f32)
        dressed(plain_ref, wide_ref, lambda part, a, b: wilson_ref[pl.ds((now * 2 + part) * 9 + a * 3 + b, 1), :], slices, now)
        insert(plain_ref, left_ref, perm_ref, turn_ref, now)


def further_kernel(slices, perm_ref, turn_ref, source_ref, moved_ref, before_ref, left_ref, wilson_ref, wide_ref, plain_ref):
    widen(source_ref, wide_ref)
    for now in range(slices):
        def link(part, a, b):
            return moved_ref[a, b, now, part : part + 1, :].astype(f32)

        def old(part, a, b):
            return before_ref[pl.ds((now * 2 + part) * 9 + a * 3 + b, 1), :]

        for a in range(3):
            for b in range(3):
                real = sum(old(0, a, m) * link(0, m, b) - old(1, a, m) * link(1, m, b) for m in range(3))
                imag = sum(old(0, a, m) * link(1, m, b) + old(1, a, m) * link(0, m, b) for m in range(3))
                wilson_ref[pl.ds(now * 18 + a * 3 + b, 1), :] = real
                wilson_ref[pl.ds(now * 18 + 9 + a * 3 + b, 1), :] = imag
        dressed(plain_ref, wide_ref, lambda part, a, b: wilson_ref[pl.ds((now * 2 + part) * 9 + a * 3 + b, 1), :], slices, now)
        insert(plain_ref, left_ref, perm_ref, turn_ref, now)


def middle_kernel(slices, left_ref, moved_ref, rows_ref, wide_ref):
    widen(moved_ref, wide_ref)
    for now in range(slices):
        meet(left_ref, wide_ref, slices, now, rows_ref, now * 16)


def last_kernel(slices, nsteps, left_ref, moved_ref, tables_ref, *rest):
    earlier, (out_ref, wide_ref, rows_ref) = rest[:nsteps], rest[nsteps:]
    widen(moved_ref, wide_ref)
    entries = 2 * nsteps + 1
    for now in range(slices):
        total = None
        rows_ref[nsteps * 8 : nsteps * 8 + 8, :] = earlier[0][now * 8 : now * 8 + 8, :]
        for reach in range(1, nsteps):
            rows_ref[(nsteps + reach) * 8 : (nsteps + reach) * 8 + 8, :] = earlier[reach][now * 16 : now * 16 + 8, :]
            rows_ref[(nsteps - reach) * 8 : (nsteps - reach) * 8 + 8, :] = earlier[reach][now * 16 + 8 : now * 16 + 16, :]
        meet(left_ref, wide_ref, slices, now, rows_ref, entries * 8)
        rows_ref[2 * nsteps * 8 : entries * 8, :] = rows_ref[entries * 8 : entries * 8 + 8, :]
        rows_ref[0:8, :] = rows_ref[entries * 8 + 8 : entries * 8 + 16, :]
        summed = jnp.sum(rows_ref[0 : entries * 8, :], axis=1, keepdims=True)
        rows_ref[0 : entries * 8, :] = jnp.broadcast_to(summed, (entries * 8, LANES))
        for l in range(entries):
            for g in range(4):
                at = ((now * entries + l) * 4 + g) * 2
                part = rows_ref[l * 8 + g : l * 8 + g + 1, :] * tables_ref[at] + rows_ref[l * 8 + 4 + g : l * 8 + 5 + g, :] * tables_ref[at + 1]
                total = part if total is None else total + part
        for row in range(tables_ref.shape[1]):
            at = now * tables_ref.shape[1] + row
            out_ref[:, at * LANES : (at + 1) * LANES] = jnp.broadcast_to(total[row : row + 1, :], (out_ref.shape[0], LANES))


def final_kernel(slices, entries, width, parts_ref, out_ref):
    peers = parts_ref.shape[0]
    sections = out_ref.shape[0] // slices
    each = peers // sections
    for section in range(sections):
        total = jnp.sum(parts_ref[section * each : (section + 1) * each, :], axis=0, keepdims=True)
        for now in range(slices):
            for entry in range(entries * 4):
                for c in range(2):
                    at = now * width + entry * 8 + c * 4
                    out_ref[section * slices + now, entry // 4, entry % 4, c : c + 1, :] = total[:, at : at + 4]


def from_behind(array, axis, by):
    peers = lax.axis_size(axis)
    return lax.ppermute(array, axis, [(i, (i + by) % peers) for i in range(peers)])


def body(propagator, links, source_z, displacements, momenta, gamma_perm, gamma_phase):
    axes = ("ta", "gz", "gy")
    sizes = tuple(lax.axis_size(a) for a in axes)
    depth_count = sizes[1]
    entries = displacements.shape[0]
    nsteps = (entries - 1) // 2
    slices = propagator.shape[4]
    sites = propagator.shape[6]
    slices_all = slices * sizes[0]
    scaling = 1.0 / (24.0 * math.sqrt(sites * sizes[2] * depth_count))
    source = jnp.reshape(jnp.transpose(propagator, (0, 2, 3, 4, 5, 1, 6)), (288 * slices, sites))
    linked = jnp.reshape(jnp.transpose(links, (1, 2, 3, 4, 0, 5)), (3, 3, slices, 2, sites))
    moved, moved_links = source, linked
    wide = pltpu.VMEM((288 * slices + 16 * slices, sites), f32)
    plain = pltpu.VMEM((slices * 8 * PAD, sites), f32)
    rows = -(-entries * 32 // LANES)
    width = rows * LANES
    peers = sizes[0] * sizes[1] * sizes[2]

    moved = from_behind(moved, "gz", -1)
    shape_left = kept((slices * 64 * PAD, sites))
    shape_wilson = kept((slices * 18, sites))
    left, first_rows, tables, wilson = pl.pallas_call(
        lambda *refs: first_kernel(slices, (slices_all, depth_count), scaling, entries, *refs),
        out_shape=(shape_left, kept((slices * 8, sites)), kept((slices * entries * 8, rows, LANES)), shape_wilson),
        in_specs=smem(5) + vmem(2),
        out_specs=tuple(vmem(4)),
        scratch_shapes=[wide, plain, pltpu.VMEM((256, sites), f32)],
        name="local",
    )(source_z, displacements, momenta, gamma_perm, gamma_phase, source, linked)
    earlier = [first_rows]
    for reach in range(1, nsteps):
        earlier.append(
            pl.pallas_call(
                lambda *refs: middle_kernel(slices, *refs),
                out_shape=kept((slices * 16, sites)),
                in_specs=vmem(2),
                out_specs=vmem(1)[0],
                scratch_shapes=[wide],
                name="middle",
            )(near(left), near(moved))
        )
        moved_links = from_behind(moved_links, "gz", -1)
        moved = from_behind(moved, "gz", -1)
        left, wilson = pl.pallas_call(
            lambda *refs: further_kernel(slices, *refs),
            out_shape=(shape_left, shape_wilson),
            in_specs=smem(2) + vmem(3),
            out_specs=tuple(vmem(2)),
            scratch_shapes=[wide, plain],
            name="further",
        )(gamma_perm, gamma_phase, source, moved_links, near(wilson))
    total = pl.pallas_call(
        lambda *refs: last_kernel(slices, nsteps, *refs),
        out_shape=kept((peers, slices * width)),
        in_specs=vmem(3 + nsteps),
        out_specs=vmem(1)[0],
        scratch_shapes=[wide, pltpu.VMEM((entries * 8 + 16, sites), f32)],
        name="last",
    )(near(left), near(moved), near(tables), *(near(e) for e in earlier))

    parts = lax.all_to_all(jnp.reshape(total, (peers, 1, slices * width)), axes, 0, 0)
    out = pl.pallas_call(
        lambda *refs: final_kernel(slices, entries, width, *refs),
        out_shape=jax.ShapeDtypeStruct((slices_all, entries, 4, 2, 4), f32),
        in_specs=vmem(1),
        name="final",
    )(near(jnp.reshape(parts, (peers, slices * width))))
    return jnp.transpose(out, (0, 1, 2, 4, 3))


def solution(mesh):
    placed = (
        P(None, None, None, None, "ta", "gz", "gy"),
        P(None, None, None, "ta", "gz", "gy"),
        P(),
        P(),
        P(),
        P(),
        P(),
    )
    return jax.shard_map(body, mesh=mesh, in_specs=placed, out_specs=P(), check_vma=False)
```

```python
import math

import jax
import jax.numpy as jnp
from jax import lax
from jax.experimental import pallas as pl
from jax.experimental.pallas import tpu as pltpu
from jax.sharding import PartitionSpec as P

f32 = jnp.float32
LANES = 128
PAD = 40


def vmem(count):
    return [pl.BlockSpec(memory_space=pltpu.VMEM) for _ in range(count)]


def near(array):
    return pltpu.with_memory_space_constraint(array, pltpu.VMEM)


def kept(shape):
    return pltpu.VMEM(shape, f32)


def smem(count):
    return [pl.BlockSpec(memory_space=pltpu.SMEM) for _ in range(count)]


def widen(packed_ref, wide_ref):
    rows = packed_ref.shape[0]
    wide_ref[0:rows, :] = packed_ref[...].astype(f32)
    wide_ref[rows:, :] = jnp.zeros((wide_ref.shape[0] - rows, wide_ref.shape[1]), f32)


def strided(wide_ref, part, spin, first, count, slices, now):
    start = ((part * 36 + first) * slices + now) * 4 + spin
    return wide_ref[pl.ds(start, count, stride=4 * slices), :]


def pair_sums(left_ref, wide_ref, slices, now, keep):
    for u in range(4):
        for s in range(4):
            real = imag = None
            for j in range(PAD // 8):
                rr = strided(wide_ref, 0, u, 8 * j, 8, slices, now)
                ri = strided(wide_ref, 1, u, 8 * j, 8, slices, now)
                lr = left_ref[pl.ds((now * 8 + s) * PAD + 8 * j, 8), :]
                li = left_ref[pl.ds((now * 8 + 4 + s) * PAD + 8 * j, 8), :]
                re = lr * rr - li * ri
                im = lr * ri + li * rr
                real = re if real is None else real + re
                imag = im if imag is None else imag + im
            keep(s, u, real, imag)


def left_rows(left_ref, now, part, s, first, value):
    left_ref[pl.ds((now * 8 + part * 4 + s) * PAD + first, value.shape[0]), :] = value


def dressed(left_ref, wide_ref, wilson, slices, now):
    zeros = jnp.zeros((PAD - 36, left_ref.shape[1]), f32)
    for s in range(4):
        for b in range(3):
            real = imag = None
            for a in range(3):
                sr = strided(wide_ref, 0, s, a * 12, 12, slices, now)
                si = strided(wide_ref, 1, s, a * 12, 12, slices, now)
                wr, wi = wilson(0, a, b), wilson(1, a, b)
                re = sr * wr + si * wi
                im = sr * wi - si * wr
                real = re if real is None else real + re
                imag = im if imag is None else imag + im
            left_rows(left_ref, now, 0, s, b * 12, real)
            left_rows(left_ref, now, 1, s, b * 12, imag)
        left_rows(left_ref, now, 0, s, 36, zeros)
        left_rows(left_ref, now, 1, s, 36, zeros)


def keep_pairs(ref, now):
    def keep(s, u, real, imag):
        ref[pl.ds((s * 4 + u) * 8, 8), :] = real
        ref[pl.ds(128 + (s * 4 + u) * 8, 8), :] = imag

    return keep


def power_of_i(turn):
    real = jnp.where(turn == 0, 1.0, jnp.where(turn == 2, -1.0, 0.0)).astype(f32)
    imag = jnp.where(turn == 1, 1.0, jnp.where(turn == 3, -1.0, 0.0)).astype(f32)
    return real, imag


def tile_at(first):
    return pl.ds(first if isinstance(first, int) else pl.multiple_of(first, 8), 8)


def insert(plain_ref, left_ref, perm_ref, turn_ref, now):
    for g in range(4):
        for s in range(4):
            u = perm_ref[g, s]
            cr, ci = power_of_i(turn_ref[g, s])
            for mirrored in range(2):
                base = (now * 2 + mirrored) * 8 + g * 2
                taken, put, sign = (u, s, -1.0) if mirrored else (s, u, 1.0)
                for j in range(PAD // 8):
                    lr = plain_ref[tile_at((now * 8 + taken) * PAD + 8 * j), :]
                    li = plain_ref[tile_at((now * 8 + 4 + taken) * PAD + 8 * j), :]
                    left_ref[tile_at((base * 4 + put) * PAD + 8 * j), :] = cr * lr - (sign * ci) * li
                    left_ref[tile_at((base * 4 + 4 + put) * PAD + 8 * j), :] = cr * li + (sign * ci) * lr


def meet(left_ref, wide_ref, slices, now, rows_ref, first):
    sums = [None] * 16
    for u in range(4):
        for j in range(PAD // 8):
            rr = strided(wide_ref, 0, u, 8 * j, 8, slices, now)
            ri = strided(wide_ref, 1, u, 8 * j, 8, slices, now)
            for which in range(8):
                base = ((now * 16 + which * 2) * 4 + u) * PAD + 8 * j
                lr = left_ref[pl.ds(base, 8), :]
                li = left_ref[pl.ds(base + 4 * PAD, 8), :]
                re = lr * rr - li * ri
                im = lr * ri + li * rr
                at = (which // 4) * 8 + which % 4
                sums[at] = re if sums[at] is None else sums[at] + re
                sums[at + 4] = im if sums[at + 4] is None else sums[at + 4] + im
    for at in range(16):
        rows_ref[pl.ds(first + at, 1), :] = jnp.sum(sums[at], axis=0, keepdims=True)


def fill_tables(tables_ref, sizes, scaling, slices, entries, source_ref, entry_ref, momenta_ref):
    slices_all, depth_count = sizes
    nsteps = (entries - 1) // 2
    rows = tables_ref.shape[1]
    depth, first_slice = lax.axis_index("gz"), lax.axis_index("ta") * slices
    lane = lax.broadcasted_iota(jnp.int32, (rows, LANES), 1)
    slot = lax.broadcasted_iota(jnp.int32, (rows, LANES), 0) * (LANES // 8) + lane // 8
    lane_part, lane_p = (lane // 4) % 2, lane % 4
    momentum = jnp.zeros((rows, LANES), jnp.int32)
    for p in range(4):
        momentum = jnp.where(lane_p == p, momenta_ref[p], momentum)
    for now in range(slices):
        origin = jnp.zeros((rows, LANES), jnp.int32)
        for p in range(4):
            origin = jnp.where(lane_p == p, source_ref[first_slice + now, p], origin)
        for l in range(entries):
            ahead = max(nsteps - l, 0)
            turn = lax.rem(momentum * (depth + ahead + depth_count - origin), depth_count)
            angle = turn.astype(f32) * (2.0 * math.pi / depth_count)
            cosine, sine = jnp.cos(angle) * scaling, jnp.sin(angle) * scaling
            first = jnp.where(lane_part == 0, cosine, -sine)
            second = jnp.where(lane_part == 0, sine, cosine)
            if l < nsteps:
                second = -second
            place = sum(jnp.where(entry_ref[j] == l, j, 0) for j in range(entries))
            for g in range(4):
                at = ((now * entries + l) * 4 + g) * 2
                tables_ref[at] = jnp.where(slot == place * 4 + g, first, 0.0)
                tables_ref[at + 1] = jnp.where(slot == place * 4 + g, second, 0.0)


def first_kernel(slices, sizes, scaling, entries, source_z_ref, entry_ref, momenta_ref, perm_ref, turn_ref, source_ref, links_ref,
                 left_ref, rows_ref, tables_ref, wilson_ref, wide_ref, plain_ref, pairs_ref):
    widen(source_ref, wide_ref)
    fill_tables(tables_ref, sizes, scaling, slices, entries, source_z_ref, entry_ref, momenta_ref)
    zeros = jnp.zeros((PAD - 36, LANES), f32)
    for now in range(slices):
        for s in range(4):
            left_rows(plain_ref, now, 0, s, 0, strided(wide_ref, 0, s, 0, 36, slices, now))
            left_rows(plain_ref, now, 1, s, 0, -strided(wide_ref, 1, s, 0, 36, slices, now))
            left_rows(plain_ref, now, 0, s, 36, zeros)
            left_rows(plain_ref, now, 1, s, 36, zeros)
        pair_sums(plain_ref, wide_ref, slices, now, keep_pairs(pairs_ref, now))
        for g in range(4):
            real = imag = None
            for s in range(4):
                at = (s * 4 + perm_ref[g, s]) * 8
                pr, pi = pairs_ref[tile_at(at), :], pairs_ref[tile_at(at + 128), :]
                cr, ci = power_of_i(turn_ref[g, s])
                re, im = cr * pr - ci * pi, cr * pi + ci * pr
                real = re if real is None else real + re
                imag = im if imag is None else imag + im
            rows_ref[now * 8 + g : now * 8 + g + 1, :] = jnp.sum(real, axis=0, keepdims=True)
            rows_ref[now * 8 + 4 + g : now * 8 + 5 + g, :] = jnp.sum(imag, axis=0, keepdims=True)
        for part in range(2):
            for a in range(3):
                for b in range(3):
                    wilson_ref[pl.ds((now * 2 + part) * 9 + a * 3 + b, 1), :] = links_ref[a, b, now, part : part + 1, :].astype(f32)
        dressed(plain_ref, wide_ref, lambda part, a, b: wilson_ref[pl.ds((now * 2 + part) * 9 + a * 3 + b, 1), :], slices, now)
        insert(plain_ref, left_ref, perm_ref, turn_ref, now)


def further_kernel(slices, perm_ref, turn_ref, source_ref, moved_ref, before_ref, left_ref, wilson_ref, wide_ref, plain_ref):
    widen(source_ref, wide_ref)
    for now in range(slices):
        def link(part, a, b):
            return moved_ref[a, b, now, part : part + 1, :].astype(f32)

        def old(part, a, b):
            return before_ref[pl.ds((now * 2 + part) * 9 + a * 3 + b, 1), :]

        for a in range(3):
            for b in range(3):
                real = sum(old(0, a, m) * link(0, m, b) - old(1, a, m) * link(1, m, b) for m in range(3))
                imag = sum(old(0, a, m) * link(1, m, b) + old(1, a, m) * link(0, m, b) for m in range(3))
                wilson_ref[pl.ds(now * 18 + a * 3 + b, 1), :] = real
                wilson_ref[pl.ds(now * 18 + 9 + a * 3 + b, 1), :] = imag
        dressed(plain_ref, wide_ref, lambda part, a, b: wilson_ref[pl.ds((now * 2 + part) * 9 + a * 3 + b, 1), :], slices, now)
        insert(plain_ref, left_ref, perm_ref, turn_ref, now)


def middle_kernel(slices, left_ref, moved_ref, rows_ref, wide_ref):
    widen(moved_ref, wide_ref)
    for now in range(slices):
        meet(left_ref, wide_ref, slices, now, rows_ref, now * 16)


def last_kernel(slices, nsteps, left_ref, moved_ref, tables_ref, *rest):
    earlier, (out_ref, wide_ref, rows_ref) = rest[:nsteps], rest[nsteps:]
    widen(moved_ref, wide_ref)
    entries = 2 * nsteps + 1
    for now in range(slices):
        total = None
        rows_ref[nsteps * 8 : nsteps * 8 + 8, :] = earlier[0][now * 8 : now * 8 + 8, :]
        for reach in range(1, nsteps):
            rows_ref[(nsteps + reach) * 8 : (nsteps + reach) * 8 + 8, :] = earlier[reach][now * 16 : now * 16 + 8, :]
            rows_ref[(nsteps - reach) * 8 : (nsteps - reach) * 8 + 8, :] = earlier[reach][now * 16 + 8 : now * 16 + 16, :]
        meet(left_ref, wide_ref, slices, now, rows_ref, entries * 8)
        rows_ref[2 * nsteps * 8 : entries * 8, :] = rows_ref[entries * 8 : entries * 8 + 8, :]
        rows_ref[0:8, :] = rows_ref[entries * 8 + 8 : entries * 8 + 16, :]
        summed = jnp.sum(rows_ref[0 : entries * 8, :], axis=1, keepdims=True)
        rows_ref[0 : entries * 8, :] = jnp.broadcast_to(summed, (entries * 8, LANES))
        for l in range(entries):
            for g in range(4):
                at = ((now * entries + l) * 4 + g) * 2
                part = rows_ref[l * 8 + g : l * 8 + g + 1, :] * tables_ref[at] + rows_ref[l * 8 + 4 + g : l * 8 + 5 + g, :] * tables_ref[at + 1]
                total = part if total is None else total + part
        for row in range(tables_ref.shape[1]):
            at = now * tables_ref.shape[1] + row
            out_ref[:, at * LANES : (at + 1) * LANES] = total[row : row + 1, :]


def final_kernel(slices, entries, width, owners, parts_ref, out_ref):
    for section in range(out_ref.shape[0] // slices):
        total = sum(parts_ref[i : i + 1, :] for i, owner in enumerate(owners) if owner == section)
        for now in range(slices):
            for entry in range(entries * 4):
                for c in range(2):
                    at = now * width + entry * 8 + c * 4
                    out_ref[section * slices + now, entry // 4, entry % 4, c : c + 1, :] = total[:, at : at + 4]


def chips_and_groups(sizes):
    nt, nz, ny = sizes
    chips = [(t, b, y) for t in range(nt) for b in range(nz // 2) for y in range(ny)]
    corner = chips[-1]
    chips.sort(key=lambda chip: (sum(abs(i - j) for i, j in zip(chip, corner)), chip))
    groups = [[(t * nz + 2 * b + (half + t + b + y) % 2) * ny + y for t, b, y in chips] for half in range(2)]
    return chips, groups


def from_behind(array, axis, by):
    peers = lax.axis_size(axis)
    return lax.ppermute(array, axis, [(i, (i + by) % peers) for i in range(peers)])


def body(propagator, links, source_z, displacements, momenta, gamma_perm, gamma_phase):
    axes = ("ta", "gz", "gy")
    sizes = tuple(lax.axis_size(a) for a in axes)
    depth_count = sizes[1]
    entries = displacements.shape[0]
    nsteps = (entries - 1) // 2
    slices = propagator.shape[4]
    sites = propagator.shape[6]
    slices_all = slices * sizes[0]
    scaling = 1.0 / (24.0 * math.sqrt(sites * sizes[2] * depth_count))
    source = jnp.reshape(jnp.transpose(propagator, (0, 2, 3, 4, 5, 1, 6)), (288 * slices, sites))
    linked = jnp.reshape(jnp.transpose(links, (1, 2, 3, 4, 0, 5)), (3, 3, slices, 2, sites))
    moved, moved_links = source, linked
    wide = pltpu.VMEM((288 * slices + 16 * slices, sites), f32)
    plain = pltpu.VMEM((slices * 8 * PAD, sites), f32)
    rows = -(-entries * 32 // LANES)
    width = rows * LANES

    moved = from_behind(moved, "gz", -1)
    shape_left = kept((slices * 64 * PAD, sites))
    shape_wilson = kept((slices * 18, sites))
    left, first_rows, tables, wilson = pl.pallas_call(
        lambda *refs: first_kernel(slices, (slices_all, depth_count), scaling, entries, *refs),
        out_shape=(shape_left, kept((slices * 8, sites)), kept((slices * entries * 8, rows, LANES)), shape_wilson),
        in_specs=smem(5) + vmem(2),
        out_specs=tuple(vmem(4)),
        scratch_shapes=[wide, plain, pltpu.VMEM((256, sites), f32)],
        name="local",
    )(source_z, displacements, momenta, gamma_perm, gamma_phase, source, linked)
    earlier = [first_rows]
    for reach in range(1, nsteps):
        earlier.append(
            pl.pallas_call(
                lambda *refs: middle_kernel(slices, *refs),
                out_shape=kept((slices * 16, sites)),
                in_specs=vmem(2),
                out_specs=vmem(1)[0],
                scratch_shapes=[wide],
                name="middle",
            )(near(left), near(moved))
        )
        moved_links = from_behind(moved_links, "gz", -1)
        moved = from_behind(moved, "gz", -1)
        left, wilson = pl.pallas_call(
            lambda *refs: further_kernel(slices, *refs),
            out_shape=(shape_left, shape_wilson),
            in_specs=smem(2) + vmem(3),
            out_specs=tuple(vmem(2)),
            scratch_shapes=[wide, plain],
            name="further",
        )(gamma_perm, gamma_phase, source, moved_links, near(wilson))
    total = pl.pallas_call(
        lambda *refs: last_kernel(slices, nsteps, *refs),
        out_shape=kept((1, slices * width)),
        in_specs=vmem(3 + nsteps),
        out_specs=vmem(1)[0],
        scratch_shapes=[wide, pltpu.VMEM((entries * 8 + 16, sites), f32)],
        name="last",
    )(near(left), near(moved), near(tables), *(near(e) for e in earlier))

    total = total + lax.ppermute(total, "gz", [(i, i ^ 1) for i in range(sizes[1])])
    chips, groups = chips_and_groups(sizes)
    copies = jnp.broadcast_to(total[None], (len(chips), 1, slices * width))
    parts = lax.all_to_all(copies, axes, 0, 0, axis_index_groups=groups)
    out = pl.pallas_call(
        lambda *refs: final_kernel(slices, entries, width, [chip[0] for chip in chips], *refs),
        out_shape=jax.ShapeDtypeStruct((slices_all, entries, 4, 2, 4), f32),
        in_specs=vmem(1),
        name="final",
    )(near(jnp.reshape(parts, (len(chips), slices * width))))
    return jnp.transpose(out, (0, 1, 2, 4, 3))


def solution(mesh):
    placed = (
        P(None, None, None, None, "ta", "gz", "gy"),
        P(None, None, None, "ta", "gz", "gy"),
        P(),
        P(),
        P(),
        P(),
        P(),
    )
    return jax.shard_map(body, mesh=mesh, in_specs=placed, out_specs=P(), check_vma=False)
```

```python
import math

import jax
import jax.numpy as jnp
from jax import lax
from jax.experimental import pallas as pl
from jax.experimental.pallas import tpu as pltpu
from jax.sharding import PartitionSpec as P

f32 = jnp.float32
LANES = 128
PAD = 40


def vmem(count):
    return [pl.BlockSpec(memory_space=pltpu.VMEM) for _ in range(count)]


def near(array):
    return pltpu.with_memory_space_constraint(array, pltpu.VMEM)


def kept(shape):
    return pltpu.VMEM(shape, f32)


def smem(count):
    return [pl.BlockSpec(memory_space=pltpu.SMEM) for _ in range(count)]


def widen(packed_ref, wide_ref):
    rows = packed_ref.shape[0]
    wide_ref[0:rows, :] = packed_ref[...].astype(f32)
    wide_ref[rows:, :] = jnp.zeros((wide_ref.shape[0] - rows, wide_ref.shape[1]), f32)


def strided(wide_ref, part, spin, first, count, slices, now):
    start = ((part * 36 + first) * slices + now) * 4 + spin
    return wide_ref[pl.ds(start, count, stride=4 * slices), :]


def pair_sums(left_ref, wide_ref, slices, now, keep):
    for u in range(4):
        for s in range(4):
            real = imag = None
            for j in range(PAD // 8):
                rr = strided(wide_ref, 0, u, 8 * j, 8, slices, now)
                ri = strided(wide_ref, 1, u, 8 * j, 8, slices, now)
                lr = left_ref[pl.ds((now * 8 + s) * PAD + 8 * j, 8), :]
                li = left_ref[pl.ds((now * 8 + 4 + s) * PAD + 8 * j, 8), :]
                re = lr * rr - li * ri
                im = lr * ri + li * rr
                real = re if real is None else real + re
                imag = im if imag is None else imag + im
            keep(s, u, real, imag)


def left_rows(left_ref, now, part, s, first, value):
    left_ref[pl.ds((now * 8 + part * 4 + s) * PAD + first, value.shape[0]), :] = value


def dressed(left_ref, wide_ref, wilson, slices, now):
    zeros = jnp.zeros((PAD - 36, left_ref.shape[1]), f32)
    for s in range(4):
        for b in range(3):
            real = imag = None
            for a in range(3):
                sr = strided(wide_ref, 0, s, a * 12, 12, slices, now)
                si = strided(wide_ref, 1, s, a * 12, 12, slices, now)
                wr, wi = wilson(0, a, b), wilson(1, a, b)
                re = sr * wr + si * wi
                im = sr * wi - si * wr
                real = re if real is None else real + re
                imag = im if imag is None else imag + im
            left_rows(left_ref, now, 0, s, b * 12, real)
            left_rows(left_ref, now, 1, s, b * 12, imag)
        left_rows(left_ref, now, 0, s, 36, zeros)
        left_rows(left_ref, now, 1, s, 36, zeros)


def keep_pairs(ref, now):
    def keep(s, u, real, imag):
        ref[pl.ds((s * 4 + u) * 8, 8), :] = real
        ref[pl.ds(128 + (s * 4 + u) * 8, 8), :] = imag

    return keep


def power_of_i(turn):
    real = jnp.where(turn == 0, 1.0, jnp.where(turn == 2, -1.0, 0.0)).astype(f32)
    imag = jnp.where(turn == 1, 1.0, jnp.where(turn == 3, -1.0, 0.0)).astype(f32)
    return real, imag


def tile_at(first):
    return pl.ds(first if isinstance(first, int) else pl.multiple_of(first, 8), 8)


def insert(plain_ref, left_ref, perm_ref, turn_ref, now):
    for g in range(4):
        for s in range(4):
            u = perm_ref[g, s]
            cr, ci = power_of_i(turn_ref[g, s])
            for mirrored in range(2):
                base = (now * 2 + mirrored) * 8 + g * 2
                taken, put, sign = (u, s, -1.0) if mirrored else (s, u, 1.0)
                for j in range(PAD // 8):
                    lr = plain_ref[tile_at((now * 8 + taken) * PAD + 8 * j), :]
                    li = plain_ref[tile_at((now * 8 + 4 + taken) * PAD + 8 * j), :]
                    left_ref[tile_at((base * 4 + put) * PAD + 8 * j), :] = cr * lr - (sign * ci) * li
                    left_ref[tile_at((base * 4 + 4 + put) * PAD + 8 * j), :] = cr * li + (sign * ci) * lr


def meet(left_ref, wide_ref, slices, now, rows_ref, first):
    sums = [None] * 16
    for u in range(4):
        for j in range(PAD // 8):
            rr = strided(wide_ref, 0, u, 8 * j, 8, slices, now)
            ri = strided(wide_ref, 1, u, 8 * j, 8, slices, now)
            for which in range(8):
                base = ((now * 16 + which * 2) * 4 + u) * PAD + 8 * j
                lr = left_ref[pl.ds(base, 8), :]
                li = left_ref[pl.ds(base + 4 * PAD, 8), :]
                re = lr * rr - li * ri
                im = lr * ri + li * rr
                at = (which // 4) * 8 + which % 4
                sums[at] = re if sums[at] is None else sums[at] + re
                sums[at + 4] = im if sums[at + 4] is None else sums[at + 4] + im
    for at in range(16):
        rows_ref[pl.ds(first + at, 1), :] = jnp.sum(sums[at], axis=0, keepdims=True)


def fill_tables(tables_ref, sizes, scaling, slices, entries, source_ref, entry_ref, momenta_ref):
    slices_all, depth_count = sizes
    nsteps = (entries - 1) // 2
    rows = tables_ref.shape[1]
    depth, first_slice = lax.axis_index("gz"), lax.axis_index("ta") * slices
    lane = lax.broadcasted_iota(jnp.int32, (rows, LANES), 1)
    slot = lax.broadcasted_iota(jnp.int32, (rows, LANES), 0) * (LANES // 8) + lane // 8
    lane_part, lane_p = (lane // 4) % 2, lane % 4
    momentum = jnp.zeros((rows, LANES), jnp.int32)
    for p in range(4):
        momentum = jnp.where(lane_p == p, momenta_ref[p], momentum)
    for now in range(slices):
        origin = jnp.zeros((rows, LANES), jnp.int32)
        for p in range(4):
            origin = jnp.where(lane_p == p, source_ref[first_slice + now, p], origin)
        for l in range(entries):
            ahead = max(nsteps - l, 0)
            turn = lax.rem(momentum * (depth + ahead + depth_count - origin), depth_count)
            angle = turn.astype(f32) * (2.0 * math.pi / depth_count)
            cosine, sine = jnp.cos(angle) * scaling, jnp.sin(angle) * scaling
            first = jnp.where(lane_part == 0, cosine, -sine)
            second = jnp.where(lane_part == 0, sine, cosine)
            if l < nsteps:
                second = -second
            place = sum(jnp.where(entry_ref[j] == l, j, 0) for j in range(entries))
            for g in range(4):
                at = ((now * entries + l) * 4 + g) * 2
                tables_ref[at] = jnp.where(slot == place * 4 + g, first, 0.0)
                tables_ref[at + 1] = jnp.where(slot == place * 4 + g, second, 0.0)


def first_kernel(slices, sizes, scaling, entries, source_z_ref, entry_ref, momenta_ref, perm_ref, turn_ref, source_ref, links_ref,
                 left_ref, rows_ref, tables_ref, wilson_ref, wide_ref, plain_ref, pairs_ref):
    widen(source_ref, wide_ref)
    fill_tables(tables_ref, sizes, scaling, slices, entries, source_z_ref, entry_ref, momenta_ref)
    zeros = jnp.zeros((PAD - 36, LANES), f32)
    for now in range(slices):
        for s in range(4):
            left_rows(plain_ref, now, 0, s, 0, strided(wide_ref, 0, s, 0, 36, slices, now))
            left_rows(plain_ref, now, 1, s, 0, -strided(wide_ref, 1, s, 0, 36, slices, now))
            left_rows(plain_ref, now, 0, s, 36, zeros)
            left_rows(plain_ref, now, 1, s, 36, zeros)
        pair_sums(plain_ref, wide_ref, slices, now, keep_pairs(pairs_ref, now))
        for g in range(4):
            real = imag = None
            for s in range(4):
                at = (s * 4 + perm_ref[g, s]) * 8
                pr, pi = pairs_ref[tile_at(at), :], pairs_ref[tile_at(at + 128), :]
                cr, ci = power_of_i(turn_ref[g, s])
                re, im = cr * pr - ci * pi, cr * pi + ci * pr
                real = re if real is None else real + re
                imag = im if imag is None else imag + im
            rows_ref[now * 8 + g : now * 8 + g + 1, :] = jnp.sum(real, axis=0, keepdims=True)
            rows_ref[now * 8 + 4 + g : now * 8 + 5 + g, :] = jnp.sum(imag, axis=0, keepdims=True)
        for part in range(2):
            for a in range(3):
                for b in range(3):
                    wilson_ref[pl.ds((now * 2 + part) * 9 + a * 3 + b, 1), :] = links_ref[a, b, now, part : part + 1, :].astype(f32)
        dressed(plain_ref, wide_ref, lambda part, a, b: wilson_ref[pl.ds((now * 2 + part) * 9 + a * 3 + b, 1), :], slices, now)
        insert(plain_ref, left_ref, perm_ref, turn_ref, now)


def further_kernel(slices, perm_ref, turn_ref, source_ref, moved_ref, before_ref, left_ref, wilson_ref, wide_ref, plain_ref):
    widen(source_ref, wide_ref)
    for now in range(slices):
        def link(part, a, b):
            return moved_ref[a, b, now, part : part + 1, :].astype(f32)

        def old(part, a, b):
            return before_ref[pl.ds((now * 2 + part) * 9 + a * 3 + b, 1), :]

        for a in range(3):
            for b in range(3):
                real = sum(old(0, a, m) * link(0, m, b) - old(1, a, m) * link(1, m, b) for m in range(3))
                imag = sum(old(0, a, m) * link(1, m, b) + old(1, a, m) * link(0, m, b) for m in range(3))
                wilson_ref[pl.ds(now * 18 + a * 3 + b, 1), :] = real
                wilson_ref[pl.ds(now * 18 + 9 + a * 3 + b, 1), :] = imag
        dressed(plain_ref, wide_ref, lambda part, a, b: wilson_ref[pl.ds((now * 2 + part) * 9 + a * 3 + b, 1), :], slices, now)
        insert(plain_ref, left_ref, perm_ref, turn_ref, now)


def middle_kernel(slices, left_ref, moved_ref, rows_ref, wide_ref):
    widen(moved_ref, wide_ref)
    for now in range(slices):
        meet(left_ref, wide_ref, slices, now, rows_ref, now * 16)


def last_kernel(slices, nsteps, left_ref, moved_ref, tables_ref, *rest):
    earlier, (out_ref, wide_ref, rows_ref) = rest[:nsteps], rest[nsteps:]
    widen(moved_ref, wide_ref)
    entries = 2 * nsteps + 1
    for now in range(slices):
        total = None
        rows_ref[nsteps * 8 : nsteps * 8 + 8, :] = earlier[0][now * 8 : now * 8 + 8, :]
        for reach in range(1, nsteps):
            rows_ref[(nsteps + reach) * 8 : (nsteps + reach) * 8 + 8, :] = earlier[reach][now * 16 : now * 16 + 8, :]
            rows_ref[(nsteps - reach) * 8 : (nsteps - reach) * 8 + 8, :] = earlier[reach][now * 16 + 8 : now * 16 + 16, :]
        meet(left_ref, wide_ref, slices, now, rows_ref, entries * 8)
        rows_ref[2 * nsteps * 8 : entries * 8, :] = rows_ref[entries * 8 : entries * 8 + 8, :]
        rows_ref[0:8, :] = rows_ref[entries * 8 + 8 : entries * 8 + 16, :]
        summed = jnp.sum(rows_ref[0 : entries * 8, :], axis=1, keepdims=True)
        rows_ref[0 : entries * 8, :] = jnp.broadcast_to(summed, (entries * 8, LANES))
        for l in range(entries):
            for g in range(4):
                at = ((now * entries + l) * 4 + g) * 2
                part = rows_ref[l * 8 + g : l * 8 + g + 1, :] * tables_ref[at] + rows_ref[l * 8 + 4 + g : l * 8 + 5 + g, :] * tables_ref[at + 1]
                total = part if total is None else total + part
        for row in range(tables_ref.shape[1]):
            at = now * tables_ref.shape[1] + row
            out_ref[:, at * LANES : (at + 1) * LANES] = total[row : row + 1, :]


def final_kernel(slices, entries, width, owners, mine_ref, other_ref, out_ref):
    for section in range(out_ref.shape[0] // slices):
        total = sum(ref[i : i + 1, :] for ref in (mine_ref, other_ref) for i, owner in enumerate(owners) if owner == section)
        for now in range(slices):
            for entry in range(entries * 4):
                for c in range(2):
                    at = now * width + entry * 8 + c * 4
                    out_ref[section * slices + now, entry // 4, entry % 4, c : c + 1, :] = total[:, at : at + 4]


def chips_and_groups(sizes):
    nt, nz, ny = sizes
    chips = [(t, b, y) for t in range(nt) for b in range(nz // 2) for y in range(ny)]
    corner = chips[-1]
    chips.sort(key=lambda chip: (sum(abs(i - j) for i, j in zip(chip, corner)), chip))
    groups = [[(t * nz + 2 * b + half) * ny + y for t, b, y in chips] for half in range(2)]
    return chips, groups


def from_behind(array, axis, by):
    peers = lax.axis_size(axis)
    return lax.ppermute(array, axis, [(i, (i + by) % peers) for i in range(peers)])


def body(propagator, links, source_z, displacements, momenta, gamma_perm, gamma_phase):
    axes = ("ta", "gz", "gy")
    sizes = tuple(lax.axis_size(a) for a in axes)
    depth_count = sizes[1]
    entries = displacements.shape[0]
    nsteps = (entries - 1) // 2
    slices = propagator.shape[4]
    sites = propagator.shape[6]
    slices_all = slices * sizes[0]
    scaling = 1.0 / (24.0 * math.sqrt(sites * sizes[2] * depth_count))
    source = jnp.reshape(jnp.transpose(propagator, (0, 2, 3, 4, 5, 1, 6)), (288 * slices, sites))
    linked = jnp.reshape(jnp.transpose(links, (1, 2, 3, 4, 0, 5)), (3, 3, slices, 2, sites))
    moved, moved_links = source, linked
    wide = pltpu.VMEM((288 * slices + 16 * slices, sites), f32)
    plain = pltpu.VMEM((slices * 8 * PAD, sites), f32)
    rows = -(-entries * 32 // LANES)
    width = rows * LANES

    moved = from_behind(moved, "gz", -1)
    shape_left = kept((slices * 64 * PAD, sites))
    shape_wilson = kept((slices * 18, sites))
    left, first_rows, tables, wilson = pl.pallas_call(
        lambda *refs: first_kernel(slices, (slices_all, depth_count), scaling, entries, *refs),
        out_shape=(shape_left, kept((slices * 8, sites)), kept((slices * entries * 8, rows, LANES)), shape_wilson),
        in_specs=smem(5) + vmem(2),
        out_specs=tuple(vmem(4)),
        scratch_shapes=[wide, plain, pltpu.VMEM((256, sites), f32)],
        name="local",
    )(source_z, displacements, momenta, gamma_perm, gamma_phase, source, linked)
    earlier = [first_rows]
    for reach in range(1, nsteps):
        earlier.append(
            pl.pallas_call(
                lambda *refs: middle_kernel(slices, *refs),
                out_shape=kept((slices * 16, sites)),
                in_specs=vmem(2),
                out_specs=vmem(1)[0],
                scratch_shapes=[wide],
                name="middle",
            )(near(left), near(moved))
        )
        moved_links = from_behind(moved_links, "gz", -1)
        moved = from_behind(moved, "gz", -1)
        left, wilson = pl.pallas_call(
            lambda *refs: further_kernel(slices, *refs),
            out_shape=(shape_left, shape_wilson),
            in_specs=smem(2) + vmem(3),
            out_specs=tuple(vmem(2)),
            scratch_shapes=[wide, plain],
            name="further",
        )(gamma_perm, gamma_phase, source, moved_links, near(wilson))
    total = pl.pallas_call(
        lambda *refs: last_kernel(slices, nsteps, *refs),
        out_shape=kept((1, slices * width)),
        in_specs=vmem(3 + nsteps),
        out_specs=vmem(1)[0],
        scratch_shapes=[wide, pltpu.VMEM((entries * 8 + 16, sites), f32)],
        name="last",
    )(near(left), near(moved), near(tables), *(near(e) for e in earlier))

    chips, groups = chips_and_groups(sizes)
    copies = jnp.broadcast_to(total[None], (len(chips), 1, slices * width))
    parts = lax.all_to_all(copies, axes, 0, 0, axis_index_groups=groups)
    mine = jnp.reshape(parts, (len(chips), slices * width))
    other = lax.ppermute(mine, "gz", [(i, i ^ 1) for i in range(sizes[1])])
    out = pl.pallas_call(
        lambda *refs: final_kernel(slices, entries, width, [chip[0] for chip in chips], *refs),
        out_shape=jax.ShapeDtypeStruct((slices_all, entries, 4, 2, 4), f32),
        in_specs=vmem(2),
        name="final",
    )(near(mine), near(other))
    return jnp.transpose(out, (0, 1, 2, 4, 3))


def solution(mesh):
    placed = (
        P(None, None, None, None, "ta", "gz", "gy"),
        P(None, None, None, "ta", "gz", "gy"),
        P(),
        P(),
        P(),
        P(),
        P(),
    )
    return jax.shard_map(body, mesh=mesh, in_specs=placed, out_specs=P(), check_vma=False)
```

```python
import math

import jax
import jax.numpy as jnp
from jax import lax
from jax.experimental import pallas as pl
from jax.experimental.pallas import tpu as pltpu
from jax.sharding import PartitionSpec as P

f32 = jnp.float32
LANES = 128
PAD = 40


def vmem(count):
    return [pl.BlockSpec(memory_space=pltpu.VMEM) for _ in range(count)]


def near(array):
    return pltpu.with_memory_space_constraint(array, pltpu.VMEM)


def kept(shape):
    return pltpu.VMEM(shape, f32)


def smem(count):
    return [pl.BlockSpec(memory_space=pltpu.SMEM) for _ in range(count)]


def widen(packed_ref, wide_ref):
    rows = packed_ref.shape[0]
    wide_ref[0:rows, :] = packed_ref[...].astype(f32)
    wide_ref[rows:, :] = jnp.zeros((wide_ref.shape[0] - rows, wide_ref.shape[1]), f32)


def strided(wide_ref, part, spin, first, count, slices, now):
    start = ((part * 36 + first) * slices + now) * 4 + spin
    return wide_ref[pl.ds(start, count, stride=4 * slices), :]


def pair_sums(left_ref, wide_ref, slices, now, keep):
    for u in range(4):
        for s in range(4):
            real = imag = None
            for j in range(PAD // 8):
                rr = strided(wide_ref, 0, u, 8 * j, 8, slices, now)
                ri = strided(wide_ref, 1, u, 8 * j, 8, slices, now)
                lr = left_ref[pl.ds((now * 8 + s) * PAD + 8 * j, 8), :]
                li = left_ref[pl.ds((now * 8 + 4 + s) * PAD + 8 * j, 8), :]
                re = lr * rr - li * ri
                im = lr * ri + li * rr
                real = re if real is None else real + re
                imag = im if imag is None else imag + im
            keep(s, u, real, imag)


def left_rows(left_ref, now, part, s, first, value):
    left_ref[pl.ds((now * 8 + part * 4 + s) * PAD + first, value.shape[0]), :] = value


def dressed(left_ref, wide_ref, wilson, slices, now):
    zeros = jnp.zeros((PAD - 36, left_ref.shape[1]), f32)
    for s in range(4):
        for b in range(3):
            real = imag = None
            for a in range(3):
                sr = strided(wide_ref, 0, s, a * 12, 12, slices, now)
                si = strided(wide_ref, 1, s, a * 12, 12, slices, now)
                wr, wi = wilson(0, a, b), wilson(1, a, b)
                re = sr * wr + si * wi
                im = sr * wi - si * wr
                real = re if real is None else real + re
                imag = im if imag is None else imag + im
            left_rows(left_ref, now, 0, s, b * 12, real)
            left_rows(left_ref, now, 1, s, b * 12, imag)
        left_rows(left_ref, now, 0, s, 36, zeros)
        left_rows(left_ref, now, 1, s, 36, zeros)


def keep_pairs(ref, now):
    def keep(s, u, real, imag):
        ref[pl.ds((s * 4 + u) * 8, 8), :] = real
        ref[pl.ds(128 + (s * 4 + u) * 8, 8), :] = imag

    return keep


def power_of_i(turn):
    real = jnp.where(turn == 0, 1.0, jnp.where(turn == 2, -1.0, 0.0)).astype(f32)
    imag = jnp.where(turn == 1, 1.0, jnp.where(turn == 3, -1.0, 0.0)).astype(f32)
    return real, imag


def tile_at(first):
    return pl.ds(first if isinstance(first, int) else pl.multiple_of(first, 8), 8)


def insert(plain_ref, left_ref, perm_ref, turn_ref, now):
    for g in range(4):
        for s in range(4):
            u = perm_ref[g, s]
            cr, ci = power_of_i(turn_ref[g, s])
            for mirrored in range(2):
                base = (now * 2 + mirrored) * 8 + g * 2
                taken, put, sign = (u, s, -1.0) if mirrored else (s, u, 1.0)
                for j in range(PAD // 8):
                    lr = plain_ref[tile_at((now * 8 + taken) * PAD + 8 * j), :]
                    li = plain_ref[tile_at((now * 8 + 4 + taken) * PAD + 8 * j), :]
                    left_ref[tile_at((base * 4 + put) * PAD + 8 * j), :] = cr * lr - (sign * ci) * li
                    left_ref[tile_at((base * 4 + 4 + put) * PAD + 8 * j), :] = cr * li + (sign * ci) * lr


def fold(tiles):
    row = lax.broadcasted_iota(jnp.int32, tiles[0].shape, 0)
    for bit in (4, 2, 1):
        half = len(tiles) // 2
        low = row & bit == 0
        tiles = [
            jnp.where(low, a + pltpu.roll(a, 8 - bit, 0), b + pltpu.roll(b, bit, 0)) for a, b in zip(tiles[:half], tiles[half:])
        ]
    return tiles[0]


def meet(left_ref, wide_ref, slices, now, rows_ref, first):
    sums = [None] * 16
    for u in range(4):
        for j in range(PAD // 8):
            rr = strided(wide_ref, 0, u, 8 * j, 8, slices, now)
            ri = strided(wide_ref, 1, u, 8 * j, 8, slices, now)
            for which in range(8):
                base = ((now * 16 + which * 2) * 4 + u) * PAD + 8 * j
                lr = left_ref[pl.ds(base, 8), :]
                li = left_ref[pl.ds(base + 4 * PAD, 8), :]
                re = lr * rr - li * ri
                im = lr * ri + li * rr
                at = (which // 4) * 8 + which % 4
                sums[at] = re if sums[at] is None else sums[at] + re
                sums[at + 4] = im if sums[at + 4] is None else sums[at + 4] + im
    rows_ref[first : first + 8, :] = fold(sums[:8])
    rows_ref[first + 8 : first + 16, :] = fold(sums[8:])


def fill_tables(tables_ref, sizes, scaling, slices, entries, source_ref, entry_ref, momenta_ref):
    _, depth_count = sizes
    nsteps = (entries - 1) // 2
    rows = tables_ref.shape[1] // LANES
    depth, first_slice = lax.axis_index("gz"), lax.axis_index("ta") * slices
    lane = lax.broadcasted_iota(jnp.int32, (8, LANES), 1)
    sub = lax.broadcasted_iota(jnp.int32, (8, LANES), 0)
    turned = 31 - lane // 4
    to_imag, lane_p = turned % 2 == 1, lane % 4
    from_imag, insertion = sub >= 4, sub % 4
    momentum = jnp.zeros((8, LANES), jnp.int32)
    for p in range(4):
        momentum = jnp.where(lane_p == p, momenta_ref[p], momentum)
    for now in range(slices):
        origin = jnp.zeros((8, LANES), jnp.int32)
        for p in range(4):
            origin = jnp.where(lane_p == p, source_ref[first_slice + now, p], origin)
        for l in range(entries):
            ahead = max(nsteps - l, 0)
            turn = lax.rem(momentum * (depth + ahead + depth_count - origin), depth_count)
            angle = turn.astype(f32) * (2.0 * math.pi / depth_count)
            cosine, sine = jnp.cos(angle) * scaling, jnp.sin(angle) * scaling
            first = jnp.where(to_imag, -sine, cosine)
            second = jnp.where(to_imag, cosine, sine)
            weight = jnp.where(from_imag, -second if l < nsteps else second, first)
            place = sum(jnp.where(entry_ref[j] == l, j, 0) for j in range(entries))
            for row in range(rows):
                hit = row * 16 + turned // 2 == place * 4 + insertion
                tables_ref[(now * entries + l) * 8 : (now * entries + l) * 8 + 8, row * LANES : (row + 1) * LANES] = jnp.where(hit, weight, 0.0)


def first_kernel(slices, sizes, scaling, entries, source_z_ref, entry_ref, momenta_ref, perm_ref, turn_ref, source_ref, links_ref,
                 left_ref, rows_ref, tables_ref, wilson_ref, wide_ref, plain_ref, pairs_ref):
    widen(source_ref, wide_ref)
    fill_tables(tables_ref, sizes, scaling, slices, entries, source_z_ref, entry_ref, momenta_ref)
    zeros = jnp.zeros((PAD - 36, LANES), f32)
    for now in range(slices):
        for s in range(4):
            left_rows(plain_ref, now, 0, s, 0, strided(wide_ref, 0, s, 0, 36, slices, now))
            left_rows(plain_ref, now, 1, s, 0, -strided(wide_ref, 1, s, 0, 36, slices, now))
            left_rows(plain_ref, now, 0, s, 36, zeros)
            left_rows(plain_ref, now, 1, s, 36, zeros)
        pair_sums(plain_ref, wide_ref, slices, now, keep_pairs(pairs_ref, now))
        for g in range(4):
            real = imag = None
            for s in range(4):
                at = (s * 4 + perm_ref[g, s]) * 8
                pr, pi = pairs_ref[tile_at(at), :], pairs_ref[tile_at(at + 128), :]
                cr, ci = power_of_i(turn_ref[g, s])
                re, im = cr * pr - ci * pi, cr * pi + ci * pr
                real = re if real is None else real + re
                imag = im if imag is None else imag + im
            rows_ref[now * 8 + g : now * 8 + g + 1, :] = jnp.sum(real, axis=0, keepdims=True)
            rows_ref[now * 8 + 4 + g : now * 8 + 5 + g, :] = jnp.sum(imag, axis=0, keepdims=True)
        for part in range(2):
            for a in range(3):
                for b in range(3):
                    wilson_ref[pl.ds((now * 2 + part) * 9 + a * 3 + b, 1), :] = links_ref[a, b, now, part : part + 1, :].astype(f32)
        dressed(plain_ref, wide_ref, lambda part, a, b: wilson_ref[pl.ds((now * 2 + part) * 9 + a * 3 + b, 1), :], slices, now)
        insert(plain_ref, left_ref, perm_ref, turn_ref, now)


def further_kernel(slices, perm_ref, turn_ref, source_ref, moved_ref, before_ref, left_ref, wilson_ref, wide_ref, plain_ref):
    widen(source_ref, wide_ref)
    for now in range(slices):
        def link(part, a, b):
            return moved_ref[a, b, now, part : part + 1, :].astype(f32)

        def old(part, a, b):
            return before_ref[pl.ds((now * 2 + part) * 9 + a * 3 + b, 1), :]

        for a in range(3):
            for b in range(3):
                real = sum(old(0, a, m) * link(0, m, b) - old(1, a, m) * link(1, m, b) for m in range(3))
                imag = sum(old(0, a, m) * link(1, m, b) + old(1, a, m) * link(0, m, b) for m in range(3))
                wilson_ref[pl.ds(now * 18 + a * 3 + b, 1), :] = real
                wilson_ref[pl.ds(now * 18 + 9 + a * 3 + b, 1), :] = imag
        dressed(plain_ref, wide_ref, lambda part, a, b: wilson_ref[pl.ds((now * 2 + part) * 9 + a * 3 + b, 1), :], slices, now)
        insert(plain_ref, left_ref, perm_ref, turn_ref, now)


def middle_kernel(slices, left_ref, moved_ref, rows_ref, wide_ref):
    widen(moved_ref, wide_ref)
    for now in range(slices):
        meet(left_ref, wide_ref, slices, now, rows_ref, now * 16)


def last_kernel(slices, nsteps, left_ref, moved_ref, tables_ref, *rest):
    earlier, (out_ref, wide_ref, rows_ref) = rest[:nsteps], rest[nsteps:]
    widen(moved_ref, wide_ref)
    entries = 2 * nsteps + 1
    width = tables_ref.shape[1]
    for now in range(slices):
        meet(left_ref, wide_ref, slices, now, rows_ref, 0)
        total = None
        for l in range(entries):
            reach = abs(l - nsteps)
            if reach == nsteps:
                rows = rows_ref[0:8, :] if l else rows_ref[8:16, :]
            elif reach:
                at = now * 16 + (0 if l > nsteps else 8)
                rows = earlier[reach][at : at + 8, :]
            else:
                rows = earlier[0][now * 8 : now * 8 + 8, :]
            summed = jnp.sum(rows, axis=1, keepdims=True)
            part = summed * tables_ref[(now * entries + l) * 8 : (now * entries + l) * 8 + 8, :]
            total = part if total is None else total + part
        out_ref[:, now * width : (now + 1) * width] = jnp.sum(total, axis=0, keepdims=True)


def final_kernel(slices, rows, owners, mine_ref, other_ref, out_ref):
    sections = out_ref.shape[0] // (slices * rows)
    each = len(owners) // sections
    width = mine_ref.shape[1] // slices
    for place in range(sections):
        picked = slice(place * each, (place + 1) * each)
        total = jnp.sum(mine_ref[picked, :] + other_ref[picked, :], axis=0, keepdims=True)
        for now in range(slices):
            for block in range(rows // 8):
                at = now * width + block // 4 * LANES
                tile = jnp.broadcast_to(total[:, at : at + LANES], (8, LANES))
                tile = pltpu.roll(tile, 4 + 32 * (block % 4), 1, stride=4, stride_axis=0)
                first = (owners[place * each] * slices + now) * rows + block * 8
                out_ref[first : first + 8, :] = tile[:, 0:4]


def chips_and_groups(sizes):
    nt, nz, ny = sizes
    chips = [(t, b, y) for t in range(nt) for b in range(nz // 2) for y in range(ny)]
    corner = chips[-1]
    chips.sort(key=lambda chip: (-chip[0], sum(abs(i - j) for i, j in zip(chip, corner)), chip))
    groups = [[(t * nz + 2 * b + half) * ny + y for t, b, y in chips] for half in range(2)]
    return chips, groups


def from_behind(array, axis, by):
    peers = lax.axis_size(axis)
    return lax.ppermute(array, axis, [(i, (i + by) % peers) for i in range(peers)])


def body(propagator, links, source_z, displacements, momenta, gamma_perm, gamma_phase):
    axes = ("ta", "gz", "gy")
    sizes = tuple(lax.axis_size(a) for a in axes)
    depth_count = sizes[1]
    entries = displacements.shape[0]
    nsteps = (entries - 1) // 2
    slices = propagator.shape[4]
    sites = propagator.shape[6]
    slices_all = slices * sizes[0]
    scaling = 1.0 / (24.0 * math.sqrt(sites * sizes[2] * depth_count))
    source = jnp.reshape(jnp.transpose(propagator, (0, 2, 3, 4, 5, 1, 6)), (288 * slices, sites))
    linked = jnp.reshape(jnp.transpose(links, (1, 2, 3, 4, 0, 5)), (3, 3, slices, 2, sites))
    moved, moved_links = source, linked
    wide = pltpu.VMEM((288 * slices + 16 * slices, sites), f32)
    plain = pltpu.VMEM((slices * 8 * PAD, sites), f32)
    rows = -(-entries * 32 // LANES)
    width = rows * LANES

    moved = from_behind(moved, "gz", -1)
    shape_left = kept((slices * 64 * PAD, sites))
    shape_wilson = kept((slices * 18, sites))
    left, first_rows, tables, wilson = pl.pallas_call(
        lambda *refs: first_kernel(slices, (slices_all, depth_count), scaling, entries, *refs),
        out_shape=(shape_left, kept((slices * 8, sites)), kept((slices * entries * 8, width)), shape_wilson),
        in_specs=smem(5) + vmem(2),
        out_specs=tuple(vmem(4)),
        scratch_shapes=[wide, plain, pltpu.VMEM((256, sites), f32)],
        name="local",
    )(source_z, displacements, momenta, gamma_perm, gamma_phase, source, linked)
    earlier = [first_rows]
    for reach in range(1, nsteps):
        earlier.append(
            pl.pallas_call(
                lambda *refs: middle_kernel(slices, *refs),
                out_shape=kept((slices * 16, sites)),
                in_specs=vmem(2),
                out_specs=vmem(1)[0],
                scratch_shapes=[wide],
                name="middle",
            )(near(left), near(moved))
        )
        moved_links = from_behind(moved_links, "gz", -1)
        moved = from_behind(moved, "gz", -1)
        left, wilson = pl.pallas_call(
            lambda *refs: further_kernel(slices, *refs),
            out_shape=(shape_left, shape_wilson),
            in_specs=smem(2) + vmem(3),
            out_specs=tuple(vmem(2)),
            scratch_shapes=[wide, plain],
            name="further",
        )(gamma_perm, gamma_phase, source, moved_links, near(wilson))
    total = pl.pallas_call(
        lambda *refs: last_kernel(slices, nsteps, *refs),
        out_shape=kept((1, slices * width)),
        in_specs=vmem(3 + nsteps),
        out_specs=vmem(1)[0],
        scratch_shapes=[wide, pltpu.VMEM((16, sites), f32)],
        name="last",
    )(near(left), near(moved), near(tables), *(near(e) for e in earlier))

    chips, groups = chips_and_groups(sizes)
    copies = jnp.broadcast_to(total[None], (len(chips), 1, slices * width))
    parts = lax.all_to_all(copies, axes, 0, 0, axis_index_groups=groups)
    mine = jnp.reshape(parts, (len(chips), slices * width))
    other = lax.ppermute(mine, "gz", [(i, i ^ 1) for i in range(sizes[1])])
    results = entries * 8
    out = pl.pallas_call(
        lambda *refs: final_kernel(slices, results, [chip[0] for chip in chips], *refs),
        out_shape=jax.ShapeDtypeStruct((slices_all * results, 4), f32),
        in_specs=vmem(2),
        name="final",
    )(near(mine), near(other))
    return jnp.transpose(jnp.reshape(out, (slices_all, entries, 4, 2, 4)), (0, 1, 2, 4, 3))


def solution(mesh):
    placed = (
        P(None, None, None, None, "ta", "gz", "gy"),
        P(None, None, None, "ta", "gz", "gy"),
        P(),
        P(),
        P(),
        P(),
        P(),
    )
    return jax.shard_map(body, mesh=mesh, in_specs=placed, out_specs=P(), check_vma=False)
```

```python
import math

import jax
import jax.numpy as jnp
from jax import lax
from jax.experimental import pallas as pl
from jax.experimental.pallas import tpu as pltpu
from jax.sharding import PartitionSpec as P

f32 = jnp.float32
LANES = 128
PAD = 40


def vmem(count):
    return [pl.BlockSpec(memory_space=pltpu.VMEM) for _ in range(count)]


def near(array):
    return pltpu.with_memory_space_constraint(array, pltpu.VMEM)


def kept(shape):
    return pltpu.VMEM(shape, f32)


def smem(count):
    return [pl.BlockSpec(memory_space=pltpu.SMEM) for _ in range(count)]


def widen(packed_ref, wide_ref):
    rows = packed_ref.shape[0]
    wide_ref[0:rows, :] = packed_ref[...].astype(f32)
    wide_ref[rows:, :] = jnp.zeros((wide_ref.shape[0] - rows, wide_ref.shape[1]), f32)


def strided(wide_ref, part, spin, first, count, slices, now):
    start = ((part * 36 + first) * slices + now) * 4 + spin
    return wide_ref[pl.ds(start, count, stride=4 * slices), :]


def pair_rows(left_ref, wide_ref, slices, now):
    tiles = []
    for u in range(4):
        sums = [None] * 8
        for j in range(PAD // 8):
            rr = strided(wide_ref, 0, u, 8 * j, 8, slices, now)
            ri = strided(wide_ref, 1, u, 8 * j, 8, slices, now)
            for s in range(4):
                lr = left_ref[pl.ds((now * 8 + s) * PAD + 8 * j, 8), :]
                li = left_ref[pl.ds((now * 8 + 4 + s) * PAD + 8 * j, 8), :]
                re = lr * rr - li * ri
                im = lr * ri + li * rr
                sums[s] = re if j == 0 else sums[s] + re
                sums[s + 4] = im if j == 0 else sums[s + 4] + im
        tiles.append(fold(sums))
    return tiles


def weighed(tiles, table):
    total = None
    for u, tile in enumerate(tiles):
        part = jnp.sum(tile, axis=1, keepdims=True) * table[u]
        total = part if total is None else total + part
    return jnp.sum(total, axis=0, keepdims=True)


def left_rows(left_ref, now, part, s, first, value):
    left_ref[pl.ds((now * 8 + part * 4 + s) * PAD + first, value.shape[0]), :] = value


def dressed(left_ref, wide_ref, wilson, slices, now):
    zeros = jnp.zeros((PAD - 36, left_ref.shape[1]), f32)
    for s in range(4):
        for b in range(3):
            real = imag = None
            for a in range(3):
                sr = strided(wide_ref, 0, s, a * 12, 12, slices, now)
                si = strided(wide_ref, 1, s, a * 12, 12, slices, now)
                wr, wi = wilson(0, a, b), wilson(1, a, b)
                re = sr * wr + si * wi
                im = sr * wi - si * wr
                real = re if real is None else real + re
                imag = im if imag is None else imag + im
            left_rows(left_ref, now, 0, s, b * 12, real)
            left_rows(left_ref, now, 1, s, b * 12, imag)
        left_rows(left_ref, now, 0, s, 36, zeros)
        left_rows(left_ref, now, 1, s, 36, zeros)


def fold(tiles):
    row = lax.broadcasted_iota(jnp.int32, tiles[0].shape, 0)
    for bit in (4, 2, 1):
        half = len(tiles) // 2
        low = row & bit == 0
        tiles = [
            jnp.where(low, a + pltpu.roll(a, 8 - bit, 0), b + pltpu.roll(b, bit, 0)) for a, b in zip(tiles[:half], tiles[half:])
        ]
    return tiles[0]


def fill_tables(sizes, scaling, slices, entries, now, source_ref, entry_ref, momenta_ref, perm_ref, turn_ref):
    depth_count = sizes[1]
    nsteps = (entries - 1) // 2
    depth, first_slice = lax.axis_index("gz"), lax.axis_index("ta") * slices
    tables = [[[] for _ in range(4)] for _ in range(nsteps + 1)]
    for row in range(-(-entries * 32 // LANES)):
        lane = lax.broadcasted_iota(jnp.int32, (8, LANES), 1)
        sub = lax.broadcasted_iota(jnp.int32, (8, LANES), 0)
        turned = 31 - lane // 4
        slot, to_imag, lane_p = row * 16 + turned // 2, turned % 2 == 1, lane % 4
        insertion, from_imag, spin = slot % 4, sub >= 4, sub % 4
        offset = jnp.full((8, LANES), -1, jnp.int32)
        for j in range(entries):
            offset = jnp.where(slot // 4 == j, entry_ref[j], offset)
        momentum = origin = jnp.zeros((8, LANES), jnp.int32)
        for p in range(4):
            momentum = jnp.where(lane_p == p, momenta_ref[p], momentum)
            origin = jnp.where(lane_p == p, source_ref[first_slice + now, p], origin)
        ahead = jnp.maximum(nsteps - offset, 0)
        angle = lax.rem(momentum * (depth + ahead + depth_count - origin), depth_count).astype(f32) * (2.0 * math.pi / depth_count)
        cosine, sine = jnp.cos(angle) * scaling, jnp.sin(angle) * scaling

        def turned_phase(turn):
            real = jnp.where(turn == 0, cosine, jnp.where(turn == 1, sine, jnp.where(turn == 2, -cosine, -sine)))
            imag = jnp.where(turn == 0, -sine, jnp.where(turn == 1, cosine, jnp.where(turn == 2, sine, -cosine)))
            return real, imag

        def by_insertion(ref, s):
            value = jnp.zeros((8, LANES), jnp.int32)
            for g in range(4):
                value = jnp.where(insertion == g, ref[g, s], value)
            return value

        columns, turns = [by_insertion(perm_ref, s) for s in range(4)], [by_insertion(turn_ref, s) for s in range(4)]
        own_column = own_turn = jnp.zeros((8, LANES), jnp.int32)
        for s in range(4):
            own_column = jnp.where(spin == s, columns[s], own_column)
            own_turn = jnp.where(spin == s, turns[s], own_turn)
        real, imag = turned_phase(own_turn)
        plain = jnp.where(to_imag, jnp.where(from_imag, real, imag), jnp.where(from_imag, -imag, real))
        for u in range(4):
            real, imag = turned_phase(turns[u])
            mirrored = jnp.where(to_imag, jnp.where(from_imag, -real, imag), jnp.where(from_imag, imag, real))
            for reach in range(nsteps + 1):
                weight = jnp.where((offset == nsteps + reach) & (own_column == u), plain, 0.0)
                if reach:
                    weight = jnp.where((offset == nsteps - reach) & (columns[u] == spin), mirrored, weight)
                tables[reach][u].append(weight)
    return tables


def first_kernel(slices, sizes, scaling, entries, source_z_ref, entry_ref, momenta_ref, perm_ref, turn_ref, source_ref, links_ref,
                 left_ref, begun_ref, tables_ref, wilson_ref, wide_ref, plain_ref):
    widen(source_ref, wide_ref)
    zeros = jnp.zeros((PAD - 36, LANES), f32)
    nsteps = (entries - 1) // 2
    width = begun_ref.shape[1] // slices
    for now in range(slices):
        tables = fill_tables(sizes, scaling, slices, entries, now, source_z_ref, entry_ref, momenta_ref, perm_ref, turn_ref)
        for reach in range(1, nsteps + 1):
            for u in range(4):
                for row, weight in enumerate(tables[reach][u]):
                    at = ((now * nsteps + reach - 1) * 4 + u) * 8
                    tables_ref[at : at + 8, row * LANES : (row + 1) * LANES] = weight
        for s in range(4):
            left_rows(plain_ref, now, 0, s, 0, strided(wide_ref, 0, s, 0, 36, slices, now))
            left_rows(plain_ref, now, 1, s, 0, -strided(wide_ref, 1, s, 0, 36, slices, now))
            left_rows(plain_ref, now, 0, s, 36, zeros)
            left_rows(plain_ref, now, 1, s, 36, zeros)
        tiles = pair_rows(plain_ref, wide_ref, slices, now)
        for row in range(width // LANES):
            at = now * width + row * LANES
            begun_ref[:, at : at + LANES] = weighed(tiles, [tables[0][u][row] for u in range(4)])
        for part in range(2):
            for a in range(3):
                for b in range(3):
                    wilson_ref[pl.ds((now * 2 + part) * 9 + a * 3 + b, 1), :] = links_ref[a, b, now, part : part + 1, :].astype(f32)
        dressed(left_ref, wide_ref, lambda part, a, b: wilson_ref[pl.ds((now * 2 + part) * 9 + a * 3 + b, 1), :], slices, now)


def further_kernel(slices, source_ref, moved_ref, before_ref, left_ref, wilson_ref, wide_ref):
    widen(source_ref, wide_ref)
    for now in range(slices):
        def link(part, a, b):
            return moved_ref[a, b, now, part : part + 1, :].astype(f32)

        def old(part, a, b):
            return before_ref[pl.ds((now * 2 + part) * 9 + a * 3 + b, 1), :]

        for a in range(3):
            for b in range(3):
                real = sum(old(0, a, m) * link(0, m, b) - old(1, a, m) * link(1, m, b) for m in range(3))
                imag = sum(old(0, a, m) * link(1, m, b) + old(1, a, m) * link(0, m, b) for m in range(3))
                wilson_ref[pl.ds(now * 18 + a * 3 + b, 1), :] = real
                wilson_ref[pl.ds(now * 18 + 9 + a * 3 + b, 1), :] = imag
        dressed(left_ref, wide_ref, lambda part, a, b: wilson_ref[pl.ds((now * 2 + part) * 9 + a * 3 + b, 1), :], slices, now)


def pairs_kernel(slices, nsteps, reach, left_ref, moved_ref, tables_ref, begun_ref, out_ref, wide_ref):
    widen(moved_ref, wide_ref)
    width = tables_ref.shape[1]
    for now in range(slices):
        tiles = pair_rows(left_ref, wide_ref, slices, now)
        first = (now * nsteps + reach - 1) * 32
        table = [tables_ref[first + 8 * u : first + 8 * u + 8, :] for u in range(4)]
        row = begun_ref[:, now * width : (now + 1) * width] + weighed(tiles, table)
        out_ref[:, now * width : (now + 1) * width] = jnp.broadcast_to(row, (out_ref.shape[0], width))


def final_kernel(slices, rows, owners, mine_ref, other_ref, out_ref):
    sections = out_ref.shape[0] // (slices * rows)
    each = len(owners) // sections
    width = mine_ref.shape[1] // slices
    for place in range(sections):
        picked = slice(place * each, (place + 1) * each)
        total = jnp.sum(mine_ref[picked, :] + other_ref[picked, :], axis=0, keepdims=True)
        for now in range(slices):
            for block in range(rows // 8):
                at = now * width + block // 4 * LANES
                tile = jnp.broadcast_to(total[:, at : at + LANES], (8, LANES))
                tile = pltpu.roll(tile, 4 + 32 * (block % 4), 1, stride=4, stride_axis=0)
                first = (owners[place * each] * slices + now) * rows + block * 8
                out_ref[first : first + 8, :] = tile[:, 0:4]


def chips_and_groups(sizes):
    nt, nz, ny = sizes
    chips = [(t, b, y) for t in range(nt) for b in range(nz // 2) for y in range(ny)]
    corner = chips[-1]
    chips.sort(key=lambda chip: (-chip[0], sum(abs(i - j) for i, j in zip(chip, corner)), chip))
    groups = [[(t * nz + 2 * b + half) * ny + y for t, b, y in chips] for half in range(2)]
    return chips, groups


def from_behind(array, axis, by):
    peers = lax.axis_size(axis)
    return lax.ppermute(array, axis, [(i, (i + by) % peers) for i in range(peers)])


def body(propagator, links, source_z, displacements, momenta, gamma_perm, gamma_phase):
    axes = ("ta", "gz", "gy")
    sizes = tuple(lax.axis_size(a) for a in axes)
    depth_count = sizes[1]
    entries = displacements.shape[0]
    nsteps = (entries - 1) // 2
    slices = propagator.shape[4]
    sites = propagator.shape[6]
    slices_all = slices * sizes[0]
    scaling = 1.0 / (24.0 * math.sqrt(sites * sizes[2] * depth_count))
    source = jnp.reshape(jnp.transpose(propagator, (0, 2, 3, 4, 5, 1, 6)), (288 * slices, sites))
    linked = jnp.reshape(jnp.transpose(links, (1, 2, 3, 4, 0, 5)), (3, 3, slices, 2, sites))
    moved, moved_links = source, linked
    wide = pltpu.VMEM((288 * slices + 16 * slices, sites), f32)
    plain = pltpu.VMEM((slices * 8 * PAD, sites), f32)
    rows = -(-entries * 32 // LANES)
    width = rows * LANES

    moved = from_behind(moved, "gz", -1)
    chips, groups = chips_and_groups(sizes)
    shape_left = kept((slices * 8 * PAD, sites))
    shape_wilson = kept((slices * 18, sites))
    left, total, tables, wilson = pl.pallas_call(
        lambda *refs: first_kernel(slices, (slices_all, depth_count), scaling, entries, *refs),
        out_shape=(shape_left, kept((1, slices * width)), kept((slices * nsteps * 32, width)), shape_wilson),
        in_specs=smem(5) + vmem(2),
        out_specs=tuple(vmem(4)),
        scratch_shapes=[wide, plain],
        name="local",
    )(source_z, displacements, momenta, gamma_perm, gamma_phase, source, linked)
    for reach in range(1, nsteps + 1):
        total = pl.pallas_call(
            lambda *refs, reach=reach: pairs_kernel(slices, nsteps, reach, *refs),
            out_shape=kept((len(chips) if reach == nsteps else 1, slices * width)),
            in_specs=vmem(4),
            out_specs=vmem(1)[0],
            scratch_shapes=[wide],
            name="pairs",
        )(near(left), near(moved), near(tables), near(total))
        if reach < nsteps:
            moved_links = from_behind(moved_links, "gz", -1)
            moved = from_behind(moved, "gz", -1)
            left, wilson = pl.pallas_call(
                lambda *refs: further_kernel(slices, *refs),
                out_shape=(shape_left, shape_wilson),
                in_specs=vmem(3),
                out_specs=tuple(vmem(2)),
                scratch_shapes=[wide],
                name="further",
            )(source, moved_links, near(wilson))
    parts = lax.all_to_all(jnp.reshape(total, (len(chips), 1, slices * width)), axes, 0, 0, axis_index_groups=groups)
    mine = jnp.reshape(parts, (len(chips), slices * width))
    other = lax.ppermute(mine, "gz", [(i, i ^ 1) for i in range(sizes[1])])
    results = entries * 8
    out = pl.pallas_call(
        lambda *refs: final_kernel(slices, results, [chip[0] for chip in chips], *refs),
        out_shape=jax.ShapeDtypeStruct((slices_all * results, 4), f32),
        in_specs=vmem(2),
        name="final",
    )(near(mine), near(other))
    return jnp.transpose(jnp.reshape(out, (slices_all, entries, 4, 2, 4)), (0, 1, 2, 4, 3))


def solution(mesh):
    placed = (
        P(None, None, None, None, "ta", "gz", "gy"),
        P(None, None, None, "ta", "gz", "gy"),
        P(),
        P(),
        P(),
        P(),
        P(),
    )
    return jax.shard_map(body, mesh=mesh, in_specs=placed, out_specs=P(), check_vma=False)
```

```python
import math

import jax
import jax.numpy as jnp
from jax import lax
from jax.experimental import pallas as pl
from jax.experimental.pallas import tpu as pltpu
from jax.sharding import PartitionSpec as P

f32 = jnp.float32
LANES = 128
PAD = 40


def vmem(count):
    return [pl.BlockSpec(memory_space=pltpu.VMEM) for _ in range(count)]


def near(array):
    return pltpu.with_memory_space_constraint(array, pltpu.VMEM)


def kept(shape):
    return pltpu.VMEM(shape, f32)


def smem(count):
    return [pl.BlockSpec(memory_space=pltpu.SMEM) for _ in range(count)]


def widen(packed_ref, wide_ref):
    rows = packed_ref.shape[0]
    wide_ref[0:rows, :] = packed_ref[...].astype(f32)
    wide_ref[rows:, :] = jnp.zeros((wide_ref.shape[0] - rows, wide_ref.shape[1]), f32)


def strided(wide_ref, part, spin, first, count, slices, now):
    start = ((part * 36 + first) * slices + now) * 4 + spin
    return wide_ref[pl.ds(start, count, stride=4 * slices), :]


def pair_rows(left_ref, wide_ref, slices, now):
    tiles = []
    for u in range(4):
        sums = [None] * 8
        for j in range(PAD // 8):
            rr = strided(wide_ref, 0, u, 8 * j, 8, slices, now)
            ri = strided(wide_ref, 1, u, 8 * j, 8, slices, now)
            for s in range(4):
                lr = left_ref[pl.ds((now * 8 + s) * PAD + 8 * j, 8), :]
                li = left_ref[pl.ds((now * 8 + 4 + s) * PAD + 8 * j, 8), :]
                re = lr * rr - li * ri
                im = lr * ri + li * rr
                sums[s] = re if j == 0 else sums[s] + re
                sums[s + 4] = im if j == 0 else sums[s + 4] + im
        tiles.append(fold(sums))
    return tiles


def weighed(tiles, table):
    total = None
    for u, tile in enumerate(tiles):
        part = jnp.sum(tile, axis=1, keepdims=True) * table[u]
        total = part if total is None else total + part
    return jnp.sum(total, axis=0, keepdims=True)


def left_rows(left_ref, now, part, s, first, value):
    left_ref[pl.ds((now * 8 + part * 4 + s) * PAD + first, value.shape[0]), :] = value


def dressed(left_ref, wide_ref, wilson, slices, now):
    zeros = jnp.zeros((PAD - 36, left_ref.shape[1]), f32)
    for s in range(4):
        for b in range(3):
            real = imag = None
            for a in range(3):
                sr = strided(wide_ref, 0, s, a * 12, 12, slices, now)
                si = strided(wide_ref, 1, s, a * 12, 12, slices, now)
                wr, wi = wilson(0, a, b), wilson(1, a, b)
                re = sr * wr + si * wi
                im = sr * wi - si * wr
                real = re if real is None else real + re
                imag = im if imag is None else imag + im
            left_rows(left_ref, now, 0, s, b * 12, real)
            left_rows(left_ref, now, 1, s, b * 12, imag)
        left_rows(left_ref, now, 0, s, 36, zeros)
        left_rows(left_ref, now, 1, s, 36, zeros)


def fold(tiles):
    row = lax.broadcasted_iota(jnp.int32, tiles[0].shape, 0)
    for bit in (4, 2, 1):
        half = len(tiles) // 2
        low = row & bit == 0
        tiles = [
            jnp.where(low, a + pltpu.roll(a, 8 - bit, 0), b + pltpu.roll(b, bit, 0)) for a, b in zip(tiles[:half], tiles[half:])
        ]
    return tiles[0]


def fill_tables(sizes, scaling, slices, entries, now, source_ref, entry_ref, momenta_ref, perm_ref, turn_ref):
    depth_count = sizes[1]
    nsteps = (entries - 1) // 2
    depth, first_slice = lax.axis_index("gz"), lax.axis_index("ta") * slices
    tables = [[[] for _ in range(4)] for _ in range(nsteps + 1)]
    for row in range(-(-entries * 32 // LANES)):
        lane = lax.broadcasted_iota(jnp.int32, (8, LANES), 1)
        sub = lax.broadcasted_iota(jnp.int32, (8, LANES), 0)
        turned = 31 - lane // 4
        slot, to_imag, lane_p = row * 16 + turned // 2, turned % 2 == 1, lane % 4
        insertion, from_imag, spin = slot % 4, sub >= 4, sub % 4
        offset = jnp.full((8, LANES), -1, jnp.int32)
        for j in range(entries):
            offset = jnp.where(slot // 4 == j, entry_ref[j], offset)
        momentum = origin = jnp.zeros((8, LANES), jnp.int32)
        for p in range(4):
            momentum = jnp.where(lane_p == p, momenta_ref[p], momentum)
            origin = jnp.where(lane_p == p, source_ref[first_slice + now, p], origin)
        ahead = jnp.maximum(nsteps - offset, 0)
        angle = lax.rem(momentum * (depth + ahead + depth_count - origin), depth_count).astype(f32) * (2.0 * math.pi / depth_count)
        cosine, sine = jnp.cos(angle) * scaling, jnp.sin(angle) * scaling

        def turned_phase(turn):
            real = jnp.where(turn == 0, cosine, jnp.where(turn == 1, sine, jnp.where(turn == 2, -cosine, -sine)))
            imag = jnp.where(turn == 0, -sine, jnp.where(turn == 1, cosine, jnp.where(turn == 2, sine, -cosine)))
            return real, imag

        def by_insertion(ref, s):
            value = jnp.zeros((8, LANES), jnp.int32)
            for g in range(4):
                value = jnp.where(insertion == g, ref[g, s], value)
            return value

        columns, turns = [by_insertion(perm_ref, s) for s in range(4)], [by_insertion(turn_ref, s) for s in range(4)]
        own_column = own_turn = jnp.zeros((8, LANES), jnp.int32)
        for s in range(4):
            own_column = jnp.where(spin == s, columns[s], own_column)
            own_turn = jnp.where(spin == s, turns[s], own_turn)
        real, imag = turned_phase(own_turn)
        plain = jnp.where(to_imag, jnp.where(from_imag, real, imag), jnp.where(from_imag, -imag, real))
        for u in range(4):
            real, imag = turned_phase(turns[u])
            mirrored = jnp.where(to_imag, jnp.where(from_imag, -real, imag), jnp.where(from_imag, imag, real))
            for reach in range(nsteps + 1):
                weight = jnp.where((offset == nsteps + reach) & (own_column == u), plain, 0.0)
                if reach:
                    weight = jnp.where((offset == nsteps - reach) & (columns[u] == spin), mirrored, weight)
                tables[reach][u].append(weight)
    return tables


def first_kernel(slices, sizes, scaling, entries, source_z_ref, entry_ref, momenta_ref, perm_ref, turn_ref, source_ref, links_ref,
                 left_ref, begun_ref, tables_ref, wilson_ref, wide_ref, plain_ref):
    widen(source_ref, wide_ref)
    zeros = jnp.zeros((PAD - 36, LANES), f32)
    nsteps = (entries - 1) // 2
    width = begun_ref.shape[1] // slices
    for now in range(slices):
        tables = fill_tables(sizes, scaling, slices, entries, now, source_z_ref, entry_ref, momenta_ref, perm_ref, turn_ref)
        for reach in range(1, nsteps + 1):
            for u in range(4):
                for row, weight in enumerate(tables[reach][u]):
                    at = ((now * nsteps + reach - 1) * 4 + u) * 8
                    tables_ref[at : at + 8, row * LANES : (row + 1) * LANES] = weight
        for s in range(4):
            left_rows(plain_ref, now, 0, s, 0, strided(wide_ref, 0, s, 0, 36, slices, now))
            left_rows(plain_ref, now, 1, s, 0, -strided(wide_ref, 1, s, 0, 36, slices, now))
            left_rows(plain_ref, now, 0, s, 36, zeros)
            left_rows(plain_ref, now, 1, s, 36, zeros)
        tiles = pair_rows(plain_ref, wide_ref, slices, now)
        for row in range(width // LANES):
            at = now * width + row * LANES
            begun_ref[:, at : at + LANES] = weighed(tiles, [tables[0][u][row] for u in range(4)])
        for part in range(2):
            for a in range(3):
                for b in range(3):
                    wilson_ref[pl.ds((now * 2 + part) * 9 + a * 3 + b, 1), :] = links_ref[a, b, now, part : part + 1, :].astype(f32)
        dressed(left_ref, wide_ref, lambda part, a, b: wilson_ref[pl.ds((now * 2 + part) * 9 + a * 3 + b, 1), :], slices, now)


def further_kernel(slices, source_ref, moved_ref, before_ref, left_ref, wilson_ref, wide_ref):
    widen(source_ref, wide_ref)
    for now in range(slices):
        def link(part, a, b):
            return moved_ref[a, b, now, part : part + 1, :].astype(f32)

        def old(part, a, b):
            return before_ref[pl.ds((now * 2 + part) * 9 + a * 3 + b, 1), :]

        for a in range(3):
            for b in range(3):
                real = sum(old(0, a, m) * link(0, m, b) - old(1, a, m) * link(1, m, b) for m in range(3))
                imag = sum(old(0, a, m) * link(1, m, b) + old(1, a, m) * link(0, m, b) for m in range(3))
                wilson_ref[pl.ds(now * 18 + a * 3 + b, 1), :] = real
                wilson_ref[pl.ds(now * 18 + 9 + a * 3 + b, 1), :] = imag
        dressed(left_ref, wide_ref, lambda part, a, b: wilson_ref[pl.ds((now * 2 + part) * 9 + a * 3 + b, 1), :], slices, now)


def pairs_kernel(slices, nsteps, reach, left_ref, moved_ref, tables_ref, begun_ref, out_ref, wide_ref):
    widen(moved_ref, wide_ref)
    width = tables_ref.shape[1]
    for now in range(slices):
        tiles = pair_rows(left_ref, wide_ref, slices, now)
        first = (now * nsteps + reach - 1) * 32
        table = [tables_ref[first + 8 * u : first + 8 * u + 8, :] for u in range(4)]
        row = begun_ref[:, now * width : (now + 1) * width] + weighed(tiles, table)
        out_ref[:, now * width : (now + 1) * width] = jnp.broadcast_to(row, (out_ref.shape[0], width))


def final_kernel(slices, rows, owners, mine_ref, other_ref, out_ref):
    sections = out_ref.shape[0] // (slices * rows)
    each = len(owners) // sections
    width = mine_ref.shape[1] // slices
    for place in range(sections):
        picked = slice(place * each, (place + 1) * each)
        total = jnp.sum(mine_ref[picked, :] + other_ref[picked, :], axis=0, keepdims=True)
        for now in range(slices):
            for block in range(rows // 8):
                at = now * width + block // 4 * LANES
                tile = jnp.broadcast_to(total[:, at : at + LANES], (8, LANES))
                tile = pltpu.roll(tile, 4 + 32 * (block % 4), 1, stride=4, stride_axis=0)
                first = (owners[place * each] * slices + now) * rows + block * 8
                out_ref[first : first + 8, :] = tile[:, 0:4]


def chips_and_groups(sizes):
    nt, nz, ny = sizes
    chips = [(t, b, y) for t in range(nt) for b in range(nz // 2) for y in range(ny)]
    groups = []
    for half in range(2):
        t, b, y = max(chips)
        leader = (t, b, max(y - half, 0))
        chips.sort(key=lambda chip: (-chip[0], sum(abs(i - j) for i, j in zip(chip, leader)), chip))
        groups.append([(t * nz + 2 * b + half) * ny + y for t, b, y in chips])
    return chips, groups


def from_behind(array, axis, by):
    peers = lax.axis_size(axis)
    return lax.ppermute(array, axis, [(i, (i + by) % peers) for i in range(peers)])


def body(propagator, links, source_z, displacements, momenta, gamma_perm, gamma_phase):
    axes = ("ta", "gz", "gy")
    sizes = tuple(lax.axis_size(a) for a in axes)
    depth_count = sizes[1]
    entries = displacements.shape[0]
    nsteps = (entries - 1) // 2
    slices = propagator.shape[4]
    sites = propagator.shape[6]
    slices_all = slices * sizes[0]
    scaling = 1.0 / (24.0 * math.sqrt(sites * sizes[2] * depth_count))
    source = jnp.reshape(jnp.transpose(propagator, (0, 2, 3, 4, 5, 1, 6)), (288 * slices, sites))
    linked = jnp.reshape(jnp.transpose(links, (1, 2, 3, 4, 0, 5)), (3, 3, slices, 2, sites))
    moved, moved_links = source, linked
    wide = pltpu.VMEM((288 * slices + 16 * slices, sites), f32)
    plain = pltpu.VMEM((slices * 8 * PAD, sites), f32)
    rows = -(-entries * 32 // LANES)
    width = rows * LANES

    moved = from_behind(moved, "gz", -1)
    chips, groups = chips_and_groups(sizes)
    shape_left = kept((slices * 8 * PAD, sites))
    shape_wilson = kept((slices * 18, sites))
    left, total, tables, wilson = pl.pallas_call(
        lambda *refs: first_kernel(slices, (slices_all, depth_count), scaling, entries, *refs),
        out_shape=(shape_left, kept((1, slices * width)), kept((slices * nsteps * 32, width)), shape_wilson),
        in_specs=smem(5) + vmem(2),
        out_specs=tuple(vmem(4)),
        scratch_shapes=[wide, plain],
        name="local",
    )(source_z, displacements, momenta, gamma_perm, gamma_phase, source, linked)
    for reach in range(1, nsteps + 1):
        total = pl.pallas_call(
            lambda *refs, reach=reach: pairs_kernel(slices, nsteps, reach, *refs),
            out_shape=kept((len(chips) if reach == nsteps else 1, slices * width)),
            in_specs=vmem(4),
            out_specs=vmem(1)[0],
            scratch_shapes=[wide],
            name="pairs",
        )(near(left), near(moved), near(tables), near(total))
        if reach < nsteps:
            moved_links = from_behind(moved_links, "gz", -1)
            moved = from_behind(moved, "gz", -1)
            left, wilson = pl.pallas_call(
                lambda *refs: further_kernel(slices, *refs),
                out_shape=(shape_left, shape_wilson),
                in_specs=vmem(3),
                out_specs=tuple(vmem(2)),
                scratch_shapes=[wide],
                name="further",
            )(source, moved_links, near(wilson))
    parts = lax.all_to_all(jnp.reshape(total, (len(chips), 1, slices * width)), axes, 0, 0, axis_index_groups=groups)
    mine = jnp.reshape(parts, (len(chips), slices * width))
    other = lax.ppermute(mine, "gz", [(i, i ^ 1) for i in range(sizes[1])])
    results = entries * 8
    out = pl.pallas_call(
        lambda *refs: final_kernel(slices, results, [chip[0] for chip in chips], *refs),
        out_shape=jax.ShapeDtypeStruct((slices_all * results, 4), f32),
        in_specs=vmem(2),
        name="final",
    )(near(mine), near(other))
    return jnp.transpose(jnp.reshape(out, (slices_all, entries, 4, 2, 4)), (0, 1, 2, 4, 3))


def solution(mesh):
    placed = (
        P(None, None, None, None, "ta", "gz", "gy"),
        P(None, None, None, "ta", "gz", "gy"),
        P(),
        P(),
        P(),
        P(),
        P(),
    )
    return jax.shard_map(body, mesh=mesh, in_specs=placed, out_specs=P(), check_vma=False)
```

```python
import math

import jax
import jax.numpy as jnp
from jax import lax
from jax.experimental import pallas as pl
from jax.experimental.pallas import tpu as pltpu
from jax.sharding import PartitionSpec as P

f32 = jnp.float32
LANES = 128
PAD = 40


def vmem(count):
    return [pl.BlockSpec(memory_space=pltpu.VMEM) for _ in range(count)]


def near(array):
    return pltpu.with_memory_space_constraint(array, pltpu.VMEM)


def kept(shape):
    return pltpu.VMEM(shape, f32)


def smem(count):
    return [pl.BlockSpec(memory_space=pltpu.SMEM) for _ in range(count)]


def widen(packed_ref, wide_ref):
    rows = packed_ref.shape[0]
    wide_ref[0:rows, :] = packed_ref[...].astype(f32)
    wide_ref[rows:, :] = jnp.zeros((wide_ref.shape[0] - rows, wide_ref.shape[1]), f32)


def strided(wide_ref, part, spin, first, count, slices, now):
    start = ((part * 36 + first) * slices + now) * 4 + spin
    return wide_ref[pl.ds(start, count, stride=4 * slices), :]


def pair_rows(left_ref, wide_ref, slices, now):
    tiles = []
    for u in range(4):
        sums = [None] * 12
        for j in range(PAD // 8):
            rr = strided(wide_ref, 0, u, 8 * j, 8, slices, now)
            ri = strided(wide_ref, 1, u, 8 * j, 8, slices, now)
            factors = (ri - rr, rr + ri, rr)
            for s in range(4):
                for part in range(3):
                    product = left_ref[pl.ds((now * 12 + part * 4 + s) * PAD + 8 * j, 8), :] * factors[part]
                    at = part * 4 + s
                    sums[at] = product if j == 0 else sums[at] + product
        sums = [sums[8 + s] - sums[4 + s] for s in range(4)] + [sums[8 + s] + sums[s] for s in range(4)]
        tiles.append(fold(sums))
    return tiles


def weighed(tiles, table):
    total = None
    for u, tile in enumerate(tiles):
        part = jnp.sum(tile, axis=1, keepdims=True) * table[u]
        total = part if total is None else total + part
    return jnp.sum(total, axis=0, keepdims=True)


def left_rows(left_ref, now, part, s, first, value):
    left_ref[pl.ds((now * 12 + part * 4 + s) * PAD + first, value.shape[0]), :] = value


def dressed(left_ref, wide_ref, wilson, slices, now):
    zeros = jnp.zeros((PAD - 36, left_ref.shape[1]), f32)
    for s in range(4):
        for b in range(3):
            real = imag = None
            for a in range(3):
                sr = strided(wide_ref, 0, s, a * 12, 12, slices, now)
                si = strided(wide_ref, 1, s, a * 12, 12, slices, now)
                wr, wi = wilson(0, a, b), wilson(1, a, b)
                re = sr * wr + si * wi
                im = sr * wi - si * wr
                real = re if real is None else real + re
                imag = im if imag is None else imag + im
            left_rows(left_ref, now, 0, s, b * 12, real)
            left_rows(left_ref, now, 1, s, b * 12, imag)
            left_rows(left_ref, now, 2, s, b * 12, real + imag)
        left_rows(left_ref, now, 0, s, 36, zeros)
        left_rows(left_ref, now, 1, s, 36, zeros)
        left_rows(left_ref, now, 2, s, 36, zeros)


def fold(tiles):
    row = lax.broadcasted_iota(jnp.int32, tiles[0].shape, 0)
    for bit in (4, 2, 1):
        half = len(tiles) // 2
        low = row & bit == 0
        tiles = [
            jnp.where(low, a + pltpu.roll(a, 8 - bit, 0), b + pltpu.roll(b, bit, 0)) for a, b in zip(tiles[:half], tiles[half:])
        ]
    return tiles[0]


def fill_tables(sizes, scaling, slices, entries, now, source_ref, entry_ref, momenta_ref, perm_ref, turn_ref):
    depth_count = sizes[1]
    nsteps = (entries - 1) // 2
    depth, first_slice = lax.axis_index("gz"), lax.axis_index("ta") * slices
    tables = [[[] for _ in range(4)] for _ in range(nsteps + 1)]
    for row in range(-(-entries * 32 // LANES)):
        lane = lax.broadcasted_iota(jnp.int32, (8, LANES), 1)
        sub = lax.broadcasted_iota(jnp.int32, (8, LANES), 0)
        turned = 31 - lane // 4
        slot, to_imag, lane_p = row * 16 + turned // 2, turned % 2 == 1, lane % 4
        insertion, from_imag, spin = slot % 4, sub >= 4, sub % 4
        offset = jnp.full((8, LANES), -1, jnp.int32)
        for j in range(entries):
            offset = jnp.where(slot // 4 == j, entry_ref[j], offset)
        momentum = origin = jnp.zeros((8, LANES), jnp.int32)
        for p in range(4):
            momentum = jnp.where(lane_p == p, momenta_ref[p], momentum)
            origin = jnp.where(lane_p == p, source_ref[first_slice + now, p], origin)
        ahead = jnp.maximum(nsteps - offset, 0)
        angle = lax.rem(momentum * (depth + ahead + depth_count - origin), depth_count).astype(f32) * (2.0 * math.pi / depth_count)
        cosine, sine = jnp.cos(angle) * scaling, jnp.sin(angle) * scaling

        def turned_phase(turn):
            real = jnp.where(turn == 0, cosine, jnp.where(turn == 1, sine, jnp.where(turn == 2, -cosine, -sine)))
            imag = jnp.where(turn == 0, -sine, jnp.where(turn == 1, cosine, jnp.where(turn == 2, sine, -cosine)))
            return real, imag

        def by_insertion(ref, s):
            value = jnp.zeros((8, LANES), jnp.int32)
            for g in range(4):
                value = jnp.where(insertion == g, ref[g, s], value)
            return value

        columns, turns = [by_insertion(perm_ref, s) for s in range(4)], [by_insertion(turn_ref, s) for s in range(4)]
        own_column = own_turn = jnp.zeros((8, LANES), jnp.int32)
        for s in range(4):
            own_column = jnp.where(spin == s, columns[s], own_column)
            own_turn = jnp.where(spin == s, turns[s], own_turn)
        real, imag = turned_phase(own_turn)
        plain = jnp.where(to_imag, jnp.where(from_imag, real, imag), jnp.where(from_imag, -imag, real))
        for u in range(4):
            real, imag = turned_phase(turns[u])
            mirrored = jnp.where(to_imag, jnp.where(from_imag, -real, imag), jnp.where(from_imag, imag, real))
            for reach in range(nsteps + 1):
                weight = jnp.where((offset == nsteps + reach) & (own_column == u), plain, 0.0)
                if reach:
                    weight = jnp.where((offset == nsteps - reach) & (columns[u] == spin), mirrored, weight)
                tables[reach][u].append(weight)
    return tables


def first_kernel(slices, sizes, scaling, entries, source_z_ref, entry_ref, momenta_ref, perm_ref, turn_ref, source_ref, links_ref,
                 left_ref, begun_ref, tables_ref, wilson_ref, wide_ref, plain_ref):
    widen(source_ref, wide_ref)
    zeros = jnp.zeros((PAD - 36, LANES), f32)
    nsteps = (entries - 1) // 2
    width = begun_ref.shape[1] // slices
    for now in range(slices):
        tables = fill_tables(sizes, scaling, slices, entries, now, source_z_ref, entry_ref, momenta_ref, perm_ref, turn_ref)
        for reach in range(1, nsteps + 1):
            for u in range(4):
                for row, weight in enumerate(tables[reach][u]):
                    at = ((now * nsteps + reach - 1) * 4 + u) * 8
                    tables_ref[at : at + 8, row * LANES : (row + 1) * LANES] = weight
        for s in range(4):
            left_rows(plain_ref, now, 0, s, 0, strided(wide_ref, 0, s, 0, 36, slices, now))
            left_rows(plain_ref, now, 1, s, 0, -strided(wide_ref, 1, s, 0, 36, slices, now))
            left_rows(plain_ref, now, 0, s, 36, zeros)
            left_rows(plain_ref, now, 1, s, 36, zeros)
            left_rows(plain_ref, now, 2, s, 36, zeros)
            left_rows(plain_ref, now, 2, s, 0, strided(wide_ref, 0, s, 0, 36, slices, now) - strided(wide_ref, 1, s, 0, 36, slices, now))
        tiles = pair_rows(plain_ref, wide_ref, slices, now)
        for row in range(width // LANES):
            at = now * width + row * LANES
            begun_ref[:, at : at + LANES] = weighed(tiles, [tables[0][u][row] for u in range(4)])
        for part in range(2):
            for a in range(3):
                for b in range(3):
                    wilson_ref[pl.ds((now * 2 + part) * 9 + a * 3 + b, 1), :] = links_ref[a, b, now, part : part + 1, :].astype(f32)
        dressed(left_ref, wide_ref, lambda part, a, b: wilson_ref[pl.ds((now * 2 + part) * 9 + a * 3 + b, 1), :], slices, now)


def further_kernel(slices, source_ref, moved_ref, before_ref, left_ref, wilson_ref, wide_ref):
    widen(source_ref, wide_ref)
    for now in range(slices):
        def link(part, a, b):
            return moved_ref[a, b, now, part : part + 1, :].astype(f32)

        def old(part, a, b):
            return before_ref[pl.ds((now * 2 + part) * 9 + a * 3 + b, 1), :]

        for a in range(3):
            for b in range(3):
                real = sum(old(0, a, m) * link(0, m, b) - old(1, a, m) * link(1, m, b) for m in range(3))
                imag = sum(old(0, a, m) * link(1, m, b) + old(1, a, m) * link(0, m, b) for m in range(3))
                wilson_ref[pl.ds(now * 18 + a * 3 + b, 1), :] = real
                wilson_ref[pl.ds(now * 18 + 9 + a * 3 + b, 1), :] = imag
        dressed(left_ref, wide_ref, lambda part, a, b: wilson_ref[pl.ds((now * 2 + part) * 9 + a * 3 + b, 1), :], slices, now)


def pairs_kernel(slices, nsteps, reach, left_ref, moved_ref, tables_ref, begun_ref, out_ref, wide_ref):
    widen(moved_ref, wide_ref)
    width = tables_ref.shape[1]
    for now in range(slices):
        tiles = pair_rows(left_ref, wide_ref, slices, now)
        first = (now * nsteps + reach - 1) * 32
        table = [tables_ref[first + 8 * u : first + 8 * u + 8, :] for u in range(4)]
        row = begun_ref[:, now * width : (now + 1) * width] + weighed(tiles, table)
        out_ref[:, now * width : (now + 1) * width] = jnp.broadcast_to(row, (out_ref.shape[0], width))


def final_kernel(slices, rows, owners, mine_ref, other_ref, out_ref):
    sections = out_ref.shape[0] // (slices * rows)
    each = len(owners) // sections
    width = mine_ref.shape[1] // slices
    for place in range(sections):
        picked = slice(place * each, (place + 1) * each)
        total = jnp.sum(mine_ref[picked, :] + other_ref[picked, :], axis=0, keepdims=True)
        for now in range(slices):
            for block in range(rows // 8):
                at = now * width + block // 4 * LANES
                tile = jnp.broadcast_to(total[:, at : at + LANES], (8, LANES))
                tile = pltpu.roll(tile, 4 + 32 * (block % 4), 1, stride=4, stride_axis=0)
                first = (owners[place * each] * slices + now) * rows + block * 8
                out_ref[first : first + 8, :] = tile[:, 0:4]


def chips_and_groups(sizes):
    nt, nz, ny = sizes
    chips = [(t, b, y) for t in range(nt) for b in range(nz // 2) for y in range(ny)]
    corner = chips[-1]
    chips.sort(key=lambda chip: (-chip[0], sum(abs(i - j) for i, j in zip(chip, corner)), chip))
    groups = [[(t * nz + 2 * b + half) * ny + y for t, b, y in chips] for half in range(2)]
    return chips, groups


def from_behind(array, axis, by):
    peers = lax.axis_size(axis)
    return lax.ppermute(array, axis, [(i, (i + by) % peers) for i in range(peers)])


def body(propagator, links, source_z, displacements, momenta, gamma_perm, gamma_phase):
    axes = ("ta", "gz", "gy")
    sizes = tuple(lax.axis_size(a) for a in axes)
    depth_count = sizes[1]
    entries = displacements.shape[0]
    nsteps = (entries - 1) // 2
    slices = propagator.shape[4]
    sites = propagator.shape[6]
    slices_all = slices * sizes[0]
    scaling = 1.0 / (24.0 * math.sqrt(sites * sizes[2] * depth_count))
    source = jnp.reshape(jnp.transpose(propagator, (0, 2, 3, 4, 5, 1, 6)), (288 * slices, sites))
    linked = jnp.reshape(jnp.transpose(links, (1, 2, 3, 4, 0, 5)), (3, 3, slices, 2, sites))
    moved, moved_links = source, linked
    wide = pltpu.VMEM((288 * slices + 16 * slices, sites), f32)
    plain = pltpu.VMEM((slices * 12 * PAD, sites), f32)
    rows = -(-entries * 32 // LANES)
    width = rows * LANES

    moved = from_behind(moved, "gz", -1)
    chips, groups = chips_and_groups(sizes)
    shape_left = kept((slices * 12 * PAD, sites))
    shape_wilson = kept((slices * 18, sites))
    left, total, tables, wilson = pl.pallas_call(
        lambda *refs: first_kernel(slices, (slices_all, depth_count), scaling, entries, *refs),
        out_shape=(shape_left, kept((1, slices * width)), kept((slices * nsteps * 32, width)), shape_wilson),
        in_specs=smem(5) + vmem(2),
        out_specs=tuple(vmem(4)),
        scratch_shapes=[wide, plain],
        name="local",
    )(source_z, displacements, momenta, gamma_perm, gamma_phase, source, linked)
    for reach in range(1, nsteps + 1):
        total = pl.pallas_call(
            lambda *refs, reach=reach: pairs_kernel(slices, nsteps, reach, *refs),
            out_shape=kept((len(chips) if reach == nsteps else 1, slices * width)),
            in_specs=vmem(4),
            out_specs=vmem(1)[0],
            scratch_shapes=[wide],
            name="pairs",
        )(near(left), near(moved), near(tables), near(total))
        if reach < nsteps:
            moved_links = from_behind(moved_links, "gz", -1)
            moved = from_behind(moved, "gz", -1)
            left, wilson = pl.pallas_call(
                lambda *refs: further_kernel(slices, *refs),
                out_shape=(shape_left, shape_wilson),
                in_specs=vmem(3),
                out_specs=tuple(vmem(2)),
                scratch_shapes=[wide],
                name="further",
            )(source, moved_links, near(wilson))
    parts = lax.all_to_all(jnp.reshape(total, (len(chips), 1, slices * width)), axes, 0, 0, axis_index_groups=groups)
    mine = jnp.reshape(parts, (len(chips), slices * width))
    other = lax.ppermute(mine, "gz", [(i, i ^ 1) for i in range(sizes[1])])
    results = entries * 8
    out = pl.pallas_call(
        lambda *refs: final_kernel(slices, results, [chip[0] for chip in chips], *refs),
        out_shape=jax.ShapeDtypeStruct((slices_all * results, 4), f32),
        in_specs=vmem(2),
        name="final",
    )(near(mine), near(other))
    return jnp.transpose(jnp.reshape(out, (slices_all, entries, 4, 2, 4)), (0, 1, 2, 4, 3))


def solution(mesh):
    placed = (
        P(None, None, None, None, "ta", "gz", "gy"),
        P(None, None, None, "ta", "gz", "gy"),
        P(),
        P(),
        P(),
        P(),
        P(),
    )
    return jax.shard_map(body, mesh=mesh, in_specs=placed, out_specs=P(), check_vma=False)
```

```python
import math

import jax
import jax.numpy as jnp
from jax import lax
from jax.experimental import pallas as pl
from jax.experimental.pallas import tpu as pltpu
from jax.sharding import PartitionSpec as P

f32 = jnp.float32
LANES = 128
PAD = 40


def vmem(count):
    return [pl.BlockSpec(memory_space=pltpu.VMEM) for _ in range(count)]


def near(array):
    return pltpu.with_memory_space_constraint(array, pltpu.VMEM)


def kept(shape):
    return pltpu.VMEM(shape, f32)


def smem(count):
    return [pl.BlockSpec(memory_space=pltpu.SMEM) for _ in range(count)]


def widen(packed_ref, wide_ref):
    rows = packed_ref.shape[0]
    wide_ref[0:rows, :] = packed_ref[...].astype(f32)
    wide_ref[rows:, :] = jnp.zeros((wide_ref.shape[0] - rows, wide_ref.shape[1]), f32)


def strided(wide_ref, part, spin, first, count, slices, now):
    start = ((part * 36 + first) * slices + now) * 4 + spin
    return wide_ref[pl.ds(start, count, stride=4 * slices), :]


def pair_rows(left_ref, wide_ref, slices, now):
    tiles = []
    for u in range(4):
        sums = [None] * 12
        for j in range(PAD // 8):
            rr = strided(wide_ref, 0, u, 8 * j, 8, slices, now)
            ri = strided(wide_ref, 1, u, 8 * j, 8, slices, now)
            factors = (ri - rr, rr + ri, rr)
            for s in range(4):
                for part in range(3):
                    product = left_ref[pl.ds((now * 12 + part * 4 + s) * PAD + 8 * j, 8), :] * factors[part]
                    at = part * 4 + s
                    sums[at] = product if j == 0 else sums[at] + product
        sums = [sums[8 + s] - sums[4 + s] for s in range(4)] + [sums[8 + s] + sums[s] for s in range(4)]
        tiles.append(fold(sums))
    return tiles


def weighed(tiles, table):
    total = None
    for u, tile in enumerate(tiles):
        part = jnp.sum(tile, axis=1, keepdims=True) * table[u]
        total = part if total is None else total + part
    return jnp.sum(total, axis=0, keepdims=True)


def left_rows(left_ref, now, part, s, first, value):
    left_ref[pl.ds((now * 12 + part * 4 + s) * PAD + first, value.shape[0]), :] = value


def dressed(left_ref, wide_ref, wilson, slices, now):
    zeros = jnp.zeros((PAD - 36, left_ref.shape[1]), f32)
    for s in range(4):
        for b in range(3):
            real = imag = None
            for a in range(3):
                sr = strided(wide_ref, 0, s, a * 12, 12, slices, now)
                si = strided(wide_ref, 1, s, a * 12, 12, slices, now)
                wr, wi = wilson(0, a, b), wilson(1, a, b)
                re = sr * wr + si * wi
                im = sr * wi - si * wr
                real = re if real is None else real + re
                imag = im if imag is None else imag + im
            left_rows(left_ref, now, 0, s, b * 12, real)
            left_rows(left_ref, now, 1, s, b * 12, imag)
            left_rows(left_ref, now, 2, s, b * 12, real + imag)
        left_rows(left_ref, now, 0, s, 36, zeros)
        left_rows(left_ref, now, 1, s, 36, zeros)
        left_rows(left_ref, now, 2, s, 36, zeros)


def fold(tiles):
    row = lax.broadcasted_iota(jnp.int32, tiles[0].shape, 0)
    for bit in (4, 2, 1):
        half = len(tiles) // 2
        low = row & bit == 0
        tiles = [
            jnp.where(low, a + pltpu.roll(a, 8 - bit, 0), b + pltpu.roll(b, bit, 0)) for a, b in zip(tiles[:half], tiles[half:])
        ]
    return tiles[0]


def fill_tables(sizes, scaling, slices, entries, now, source_ref, entry_ref, momenta_ref, perm_ref, turn_ref):
    depth_count = sizes[1]
    nsteps = (entries - 1) // 2
    depth, first_slice = lax.axis_index("gz"), lax.axis_index("ta") * slices
    tables = [[[] for _ in range(4)] for _ in range(nsteps + 1)]
    for row in range(-(-entries * 32 // LANES)):
        lane = lax.broadcasted_iota(jnp.int32, (8, LANES), 1)
        sub = lax.broadcasted_iota(jnp.int32, (8, LANES), 0)
        turned = 31 - lane // 4
        slot, to_imag, lane_p = row * 16 + turned // 2, turned % 2 == 1, lane % 4
        insertion, from_imag, spin = slot % 4, sub >= 4, sub % 4
        offset = jnp.full((8, LANES), -1, jnp.int32)
        for j in range(entries):
            offset = jnp.where(slot // 4 == j, entry_ref[j], offset)
        momentum = origin = jnp.zeros((8, LANES), jnp.int32)
        for p in range(4):
            momentum = jnp.where(lane_p == p, momenta_ref[p], momentum)
            origin = jnp.where(lane_p == p, source_ref[first_slice + now, p], origin)
        ahead = jnp.maximum(nsteps - offset, 0)
        angle = lax.rem(momentum * (depth + ahead + depth_count - origin), depth_count).astype(f32) * (2.0 * math.pi / depth_count)
        cosine, sine = jnp.cos(angle) * scaling, jnp.sin(angle) * scaling

        def turned_phase(turn):
            real = jnp.where(turn == 0, cosine, jnp.where(turn == 1, sine, jnp.where(turn == 2, -cosine, -sine)))
            imag = jnp.where(turn == 0, -sine, jnp.where(turn == 1, cosine, jnp.where(turn == 2, sine, -cosine)))
            return real, imag

        def by_insertion(ref, s):
            value = jnp.zeros((8, LANES), jnp.int32)
            for g in range(4):
                value = jnp.where(insertion == g, ref[g, s], value)
            return value

        columns, turns = [by_insertion(perm_ref, s) for s in range(4)], [by_insertion(turn_ref, s) for s in range(4)]
        own_column = own_turn = jnp.zeros((8, LANES), jnp.int32)
        for s in range(4):
            own_column = jnp.where(spin == s, columns[s], own_column)
            own_turn = jnp.where(spin == s, turns[s], own_turn)
        real, imag = turned_phase(own_turn)
        plain = jnp.where(to_imag, jnp.where(from_imag, real, imag), jnp.where(from_imag, -imag, real))
        for u in range(4):
            real, imag = turned_phase(turns[u])
            mirrored = jnp.where(to_imag, jnp.where(from_imag, -real, imag), jnp.where(from_imag, imag, real))
            for reach in range(nsteps + 1):
                weight = jnp.where((offset == nsteps + reach) & (own_column == u), plain, 0.0)
                if reach:
                    weight = jnp.where((offset == nsteps - reach) & (columns[u] == spin), mirrored, weight)
                tables[reach][u].append(weight)
    return tables


def first_kernel(slices, sizes, scaling, entries, source_z_ref, entry_ref, momenta_ref, perm_ref, turn_ref, source_ref, links_ref,
                 left_ref, begun_ref, tables_ref, wilson_ref, wide_ref, plain_ref):
    widen(source_ref, wide_ref)
    zeros = jnp.zeros((PAD - 36, LANES), f32)
    nsteps = (entries - 1) // 2
    width = begun_ref.shape[1] // slices
    for now in range(slices):
        tables = fill_tables(sizes, scaling, slices, entries, now, source_z_ref, entry_ref, momenta_ref, perm_ref, turn_ref)
        for reach in range(1, nsteps + 1):
            for u in range(4):
                for row, weight in enumerate(tables[reach][u]):
                    at = ((now * nsteps + reach - 1) * 4 + u) * 8
                    tables_ref[at : at + 8, row * LANES : (row + 1) * LANES] = weight
        for s in range(4):
            left_rows(plain_ref, now, 0, s, 0, strided(wide_ref, 0, s, 0, 36, slices, now))
            left_rows(plain_ref, now, 1, s, 0, -strided(wide_ref, 1, s, 0, 36, slices, now))
            left_rows(plain_ref, now, 0, s, 36, zeros)
            left_rows(plain_ref, now, 1, s, 36, zeros)
            left_rows(plain_ref, now, 2, s, 36, zeros)
            left_rows(plain_ref, now, 2, s, 0, strided(wide_ref, 0, s, 0, 36, slices, now) - strided(wide_ref, 1, s, 0, 36, slices, now))
        tiles = pair_rows(plain_ref, wide_ref, slices, now)
        for row in range(width // LANES):
            at = now * width + row * LANES
            begun_ref[:, at : at + LANES] = weighed(tiles, [tables[0][u][row] for u in range(4)])
        for part in range(2):
            for a in range(3):
                for b in range(3):
                    wilson_ref[pl.ds((now * 2 + part) * 9 + a * 3 + b, 1), :] = links_ref[a, b, now, part : part + 1, :].astype(f32)
        dressed(left_ref, wide_ref, lambda part, a, b: wilson_ref[pl.ds((now * 2 + part) * 9 + a * 3 + b, 1), :], slices, now)


def further_kernel(slices, source_ref, moved_ref, before_ref, left_ref, wilson_ref, wide_ref):
    widen(source_ref, wide_ref)
    for now in range(slices):
        def link(part, a, b):
            return moved_ref[a, b, now, part : part + 1, :].astype(f32)

        def old(part, a, b):
            return before_ref[pl.ds((now * 2 + part) * 9 + a * 3 + b, 1), :]

        for a in range(3):
            for b in range(3):
                real = sum(old(0, a, m) * link(0, m, b) - old(1, a, m) * link(1, m, b) for m in range(3))
                imag = sum(old(0, a, m) * link(1, m, b) + old(1, a, m) * link(0, m, b) for m in range(3))
                wilson_ref[pl.ds(now * 18 + a * 3 + b, 1), :] = real
                wilson_ref[pl.ds(now * 18 + 9 + a * 3 + b, 1), :] = imag
        dressed(left_ref, wide_ref, lambda part, a, b: wilson_ref[pl.ds((now * 2 + part) * 9 + a * 3 + b, 1), :], slices, now)


def pairs_kernel(slices, nsteps, reach, left_ref, moved_ref, tables_ref, begun_ref, out_ref, wide_ref):
    widen(moved_ref, wide_ref)
    width = tables_ref.shape[1]
    for now in range(slices):
        tiles = pair_rows(left_ref, wide_ref, slices, now)
        first = (now * nsteps + reach - 1) * 32
        table = [tables_ref[first + 8 * u : first + 8 * u + 8, :] for u in range(4)]
        row = begun_ref[:, now * width : (now + 1) * width] + weighed(tiles, table)
        out_ref[:, now * width : (now + 1) * width] = jnp.broadcast_to(row, (out_ref.shape[0], width))


def final_kernel(slices, rows, owners, mine_ref, other_ref, out_ref):
    sections = out_ref.shape[0] // (slices * rows)
    each = len(owners) // sections
    width = mine_ref.shape[1] // slices
    for place in range(sections):
        picked = slice(place * each, (place + 1) * each)
        total = jnp.sum(mine_ref[picked, :] + other_ref[picked, :], axis=0, keepdims=True)
        for now in range(slices):
            for block in range(rows // 8):
                at = now * width + block // 4 * LANES
                tile = jnp.broadcast_to(total[:, at : at + LANES], (8, LANES))
                tile = pltpu.roll(tile, 4 + 32 * (block % 4), 1, stride=4, stride_axis=0)
                first = (owners[place * each] * slices + now) * rows + block * 8
                out_ref[first : first + 8, :] = tile[:, 0:4]


def chips_and_groups(sizes):
    nt, nz, ny = sizes
    chips = [(t, b, y) for t in range(nt) for b in range(nz // 2) for y in range(ny)]
    groups = []
    for half in range(2):
        t, b, y = max(chips)
        leader = (t, b, max(y - half, 0))
        chips.sort(key=lambda chip: (-chip[0], sum(abs(i - j) for i, j in zip(chip, leader)), chip))
        groups.append([(t * nz + 2 * b + half) * ny + y for t, b, y in chips])
    return chips, groups


def from_behind(array, axis, by):
    peers = lax.axis_size(axis)
    return lax.ppermute(array, axis, [(i, (i + by) % peers) for i in range(peers)])


def body(propagator, links, source_z, displacements, momenta, gamma_perm, gamma_phase):
    axes = ("ta", "gz", "gy")
    sizes = tuple(lax.axis_size(a) for a in axes)
    depth_count = sizes[1]
    entries = displacements.shape[0]
    nsteps = (entries - 1) // 2
    slices = propagator.shape[4]
    sites = propagator.shape[6]
    slices_all = slices * sizes[0]
    scaling = 1.0 / (24.0 * math.sqrt(sites * sizes[2] * depth_count))
    source = jnp.reshape(jnp.transpose(propagator, (0, 2, 3, 4, 5, 1, 6)), (288 * slices, sites))
    linked = jnp.reshape(jnp.transpose(links, (1, 2, 3, 4, 0, 5)), (3, 3, slices, 2, sites))
    moved, moved_links = source, linked
    wide = pltpu.VMEM((288 * slices + 16 * slices, sites), f32)
    plain = pltpu.VMEM((slices * 12 * PAD, sites), f32)
    rows = -(-entries * 32 // LANES)
    width = rows * LANES

    moved = from_behind(moved, "gz", -1)
    chips, groups = chips_and_groups(sizes)
    shape_left = kept((slices * 12 * PAD, sites))
    shape_wilson = kept((slices * 18, sites))
    left, total, tables, wilson = pl.pallas_call(
        lambda *refs: first_kernel(slices, (slices_all, depth_count), scaling, entries, *refs),
        out_shape=(shape_left, kept((1, slices * width)), kept((slices * nsteps * 32, width)), shape_wilson),
        in_specs=smem(5) + vmem(2),
        out_specs=tuple(vmem(4)),
        scratch_shapes=[wide, plain],
        name="local",
    )(source_z, displacements, momenta, gamma_perm, gamma_phase, source, linked)
    for reach in range(1, nsteps + 1):
        total = pl.pallas_call(
            lambda *refs, reach=reach: pairs_kernel(slices, nsteps, reach, *refs),
            out_shape=kept((len(chips) if reach == nsteps else 1, slices * width)),
            in_specs=vmem(4),
            out_specs=vmem(1)[0],
            scratch_shapes=[wide],
            name="pairs",
        )(near(left), near(moved), near(tables), near(total))
        if reach < nsteps:
            moved_links = from_behind(moved_links, "gz", -1)
            moved = from_behind(moved, "gz", -1)
            left, wilson = pl.pallas_call(
                lambda *refs: further_kernel(slices, *refs),
                out_shape=(shape_left, shape_wilson),
                in_specs=vmem(3),
                out_specs=tuple(vmem(2)),
                scratch_shapes=[wide],
                name="further",
            )(source, moved_links, near(wilson))
    parts = lax.all_to_all(jnp.reshape(total, (len(chips), 1, slices * width)), axes, 0, 0, axis_index_groups=groups)
    mine = jnp.reshape(parts, (len(chips), slices * width))
    other = lax.ppermute(mine, "gz", [(i, i ^ 1) for i in range(sizes[1])])
    results = entries * 8
    out = pl.pallas_call(
        lambda *refs: final_kernel(slices, results, [chip[0] for chip in chips], *refs),
        out_shape=jax.ShapeDtypeStruct((slices_all * results, 4), f32),
        in_specs=vmem(2),
        name="final",
    )(near(mine), near(other))
    return jnp.transpose(jnp.reshape(out, (slices_all, entries, 4, 2, 4)), (0, 1, 2, 4, 3))


def solution(mesh):
    placed = (
        P(None, None, None, None, "ta", "gz", "gy"),
        P(None, None, None, "ta", "gz", "gy"),
        P(),
        P(),
        P(),
        P(),
        P(),
    )
    return jax.shard_map(body, mesh=mesh, in_specs=placed, out_specs=P(), check_vma=False)
```
